256 devices in a mesh: gx: 16 (over y, x), gy: 8 (over z_hi, core), gz: 2 (over z_lo).
Axes of the slice: x: 4, y: 4, z: 8 (z_hi: 4, z_lo: 2; z = z_hi * 2 + z_lo), core: 2. Of those that a mesh axis runs over, the one named last changes fastest.
Arguments:
- head: float32 [16, 1024, 2048], P('gz', 'gx', 'gy'), may hold values from -2 to -0.2
- soil: int32 [16, 1024, 2048], P('gz', 'gx', 'gy'), may hold values from 0 to 7
- boundary: int32 [16, 1024, 2048], P('gz', 'gx', 'gy'), may hold values 0 or 1
- rhs: float32 [16, 1024, 2048], P('gz', 'gx', 'gy'), may hold values from -6 to 6
- soil_alpha: float32 [8], replicated, may hold values from 0.5 to 4
- soil_n: float32 [8], replicated, may hold values from 1.4 to 3
- soil_ks: float32 [8], replicated, may hold values from 0.1 to 2
Outputs:
- update: float32 [16, 1024, 2048], P('gz', 'gx', 'gy')
- residual: float32 [16, 1024, 2048], P('gz', 'gx', 'gy')
The draws below stay inside these ranges and needn't reach their ends.
Inputs may be any that keep to these rules, and one draw needn't show every extreme that they name: soil indexes the tables soil_alpha, soil_n and soil_ks.
All inputs are finite; a program needn't handle non-finite values. No bound on the sum of `boundary` on one device may be relied on, other than what follows from the above.
Results may differ from the reference program's by a relative error of at most 0.0003.
Values sent between devices are 32-bit elements; how exact they have to be, the bound alone decides.
No kernel may reach another device: no remote copies, remote signals or barrier semaphores. Data moves between devices by JAX's collectives and lax.ppermute only.
A program may use at most 128 MiB of HBM per device.

```python
import math
import jax
import jax.numpy as jnp

ITERS = 2
SOILS = 8
NZ = 16
NX = 1024
NY = 2048


def plant(array, key, smallest, high):
    place = [jax.random.randint(jax.random.fold_in(key, axis), (), 0, length) for axis, length in enumerate(array.shape)]
    main_axis = array.shape.index(max(array.shape))
    neighbour = place[:main_axis] + [(place[main_axis] + 1) % array.shape[main_axis]] + place[main_axis + 1:]
    return array.at[tuple(place)].set(smallest).at[tuple(neighbour)].set(high)


def level_of(key, shape, shards, least, largest):
    def one(position, parts):
        draws = jax.random.uniform(jax.random.fold_in(jax.random.fold_in(key, 6), position), (parts,), jnp.float32, least / len(shards), largest / len(shards))
        return jnp.repeat(jnp.exp(draws), shape[position] // parts).reshape((-1,) + (1,) * (len(shape) - position - 1))

    loudness = one(*shards[0])
    for cut in shards[1:]:
        loudness = loudness * one(*cut)
    return loudness


def noise(stream_key, shape, scale, reach, cuts=(), kind=jnp.bfloat16):
    values = scale * jax.random.normal(stream_key, shape, jnp.float32)
    if cuts:
        values = values * level_of(stream_key, shape, cuts, -0.22, 0.18)
    return jnp.clip(values, -reach, reach).astype(kind)


def setup_inputs(seed: int = 0) -> dict:
    splits = jax.random.split(jax.random.key(seed), 8)
    head = jnp.clip(-2.0 + 1.8 * jax.random.uniform(splits[0], (NZ, NX, NY), jnp.float32) ** level_of(splits[0], (NZ, NX, NY), ((0, 2), (1, 16), (2, 8)), -0.2, 0.2), -2.0, -0.2)
    soil = plant(jax.random.randint(splits[1], (NZ, NX, NY), 0, SOILS), jax.random.fold_in(splits[1], 1), 0, SOILS - 1).astype(jnp.int32)
    boundary = plant((jax.random.randint(splits[2], (NZ, NX, NY), 0, 16) < 1).astype(jnp.int32), jax.random.fold_in(splits[2], 1), 0, 1)
    rhs = noise(splits[3], (NZ, NX, NY), 1.0, 6.0, ((0, 2), (1, 16), (2, 8)), jnp.float32)
    soil_alpha = jnp.clip(jnp.exp(jax.random.uniform(splits[4], (SOILS,), jnp.float32, math.log(0.5), math.log(4.0))), 0.5, 4.0)
    soil_n = jnp.clip(jax.random.uniform(splits[5], (SOILS,), jnp.float32, 1.4, 3.0), 1.4, 3.0)
    soil_ks = jnp.clip(jnp.exp(jax.random.uniform(splits[6], (SOILS,), jnp.float32, math.log(0.1), math.log(2.0))), 0.1, 2.0)
    return dict(head=head, soil=soil, boundary=boundary, rhs=rhs, soil_alpha=soil_alpha, soil_n=soil_n, soil_ks=soil_ks)


EPS = 1e-06
SPEC = 0.0001
PORE = 0.4
STEP = 0.25

def lookup(soil, table):
    picked = jnp.zeros(soil.shape, table.dtype)
    for entry in range(table.shape[0]):
        picked = picked + jnp.where(soil == entry, table[entry], jnp.zeros((), table.dtype))
    return picked

def retention(level, alpha, expo):
    power = 1.0 - 1.0 / expo
    ratio = jnp.power(alpha * -level, expo)
    sat = jnp.power(1.0 + ratio, -power)
    rel = jnp.sqrt(sat) * jnp.square(1.0 - jnp.power(ratio / (1.0 + ratio), power))
    return (sat, rel)

def cell_terms(head, soil, soil_alpha, soil_n, soil_ks):
    alpha = lookup(soil, soil_alpha)
    expo = lookup(soil, soil_n)
    satcond = lookup(soil, soil_ks)

    def curve(level):
        return retention(level, alpha, expo)
    (sat, rel), pullback = jax.vjp(curve, head)
    unity = jnp.ones_like(head)
    nothing = jnp.zeros_like(head)
    dsat = pullback((unity, nothing))[0]
    drel = pullback((nothing, unity))[0]
    capacity = (SPEC * sat + PORE * dsat) / STEP
    return (jnp.stack([satcond * rel, satcond * drel, head]), capacity)

def faces_of(padded, direction, start):
    extent = padded.shape[padded.ndim - 3 + direction] - 2
    window = [slice(1, -1), slice(1, -1), slice(1, -1)]
    window[direction] = slice(start, start + extent + 1)
    return padded[..., window[0], window[1], window[2]]

def apply_jacobian(moved, coeffs, capacity, boundary):
    field = moved[1:-1, 1:-1, 1:-1]
    result = capacity * field
    for direction, upward in ((0, 1.0), (1, 0.0), (2, 0.0)):
        lower = faces_of(coeffs, direction, 0)
        upper = faces_of(coeffs, direction, 1)
        v_lo = faces_of(moved, direction, 0)
        v_hi = faces_of(moved, direction, 1)
        k_lo, dk_lo, h_lo = (lower[0], lower[1], lower[2])
        k_hi, dk_hi, h_hi = (upper[0], upper[1], upper[2])
        summed = k_lo + k_hi
        harmonic = 2.0 * k_lo * k_hi / summed
        slope = h_lo - h_hi - upward
        squared = summed * summed
        weight_lo = 2.0 * k_hi * k_hi / squared
        weight_hi = 2.0 * k_lo * k_lo / squared
        flux = harmonic * (v_lo - v_hi) + slope * (weight_lo * dk_lo * v_lo + weight_hi * dk_hi * v_hi)
        result = result + jnp.diff(flux, axis=direction)
    return jnp.where(boundary == 1, field, result)

def least_squares(hess, beta):
    count = len(hess)
    columns = []
    for column in range(count):
        entries = []
        for row in range(count + 1):
            entries.append(hess[column][row] if row <= column + 1 else jnp.zeros((), beta.dtype))
        columns.append(jnp.stack(entries))
    basis_q = []
    upper_r = [[None] * count for row in range(count)]
    for column in range(count):
        vector = columns[column]
        for row in range(column):
            upper_r[row][column] = jnp.sum(basis_q[row] * columns[column])
        for row in range(column):
            vector = vector - upper_r[row][column] * basis_q[row]
        upper_r[column][column] = jnp.sqrt(jnp.sum(vector * vector))
        basis_q.append(vector / upper_r[column][column])
    target = [beta * basis_q[row][0] for row in range(count)]
    solved = [None] * count
    for row in range(count - 1, -1, -1):
        value = target[row]
        for column in range(row + 1, count):
            value = value - upper_r[row][column] * solved[column]
        solved[row] = value / upper_r[row][row]
    return solved

def reference(head, soil, boundary, rhs, soil_alpha, soil_n, soil_ks):
    stacked, capacity = cell_terms(head, soil, soil_alpha, soil_n, soil_ks)
    coeffs = jnp.pad(stacked, ((0, 0), (1, 1), (1, 1), (1, 1)))

    def jacobian(field):
        return apply_jacobian(jnp.pad(field, 1), coeffs, capacity, boundary)
    beta = jnp.sqrt(jnp.sum(rhs * rhs) + EPS)
    basis = [rhs / beta]
    hess = []
    for column in range(ITERS):
        image = jacobian(basis[column])
        projected = [jnp.sum(image * vector) for vector in basis]
        rest = image
        for index_row in range(len(basis)):
            rest = rest - projected[index_row] * basis[index_row]
        length = jnp.sqrt(jnp.sum(rest * rest) + EPS)
        basis.append(rest / length)
        hess.append(projected + [length])
    solved = least_squares(hess, beta)
    update = solved[0] * basis[0]
    for column in range(1, ITERS):
        update = update + solved[column] * basis[column]
    residual = rhs - jacobian(update)
    return (update, residual)
```

```python
import jax
import jax.numpy as jnp
from jax import lax
from jax.experimental import pallas as pl
from jax.experimental.pallas import tpu as pltpu
from jax.sharding import Mesh
from jax.sharding import PartitionSpec as P

AXES = ("gx_0", "gx_1", "gy_0", "gy_1", "gz")
GX = ("gx_0", "gx_1")
GY = ("gy_0", "gy_1")
SOILS = 8
EPS = 1e-06
SPEC = 0.0001
PORE = 0.4
STEP = 0.25
F32 = jnp.float32
NZ, NX, NY = 8, 64, 256
BLOCK = (NZ, NX, NY)
TILES = NX // 8
PARAMS = pltpu.CompilerParams(vmem_limit_bytes=24 * 1024 * 1024)
VMEM = pl.BlockSpec(memory_space=pltpu.VMEM)
SMEM = pl.BlockSpec(memory_space=pltpu.SMEM)


def shape(*dims):
    return jax.ShapeDtypeStruct(dims, F32)


def along(axes):
    index = lax.axis_index(axes[0])
    return index * lax.axis_size(axes[1]) + lax.axis_index(axes[1])


def cell_terms(head, soil, alpha_ref, n_ref, ks_ref):
    alpha = jnp.full(head.shape, alpha_ref[0], F32)
    expo = jnp.full(head.shape, n_ref[0], F32)
    ks = jnp.full(head.shape, ks_ref[0], F32)
    for entry in range(1, SOILS):
        here = soil == entry
        alpha = jnp.where(here, alpha_ref[entry], alpha)
        expo = jnp.where(here, n_ref[entry], expo)
        ks = jnp.where(here, ks_ref[entry], ks)
    depth = -head
    power = 1.0 - 1.0 / expo
    scaled = expo * jnp.log(alpha * depth)
    inverse = jnp.exp(-scaled)
    total = 1.0 + inverse
    part = jnp.log(total)
    root = jnp.exp((-0.5 * power) * (part + scaled))
    bent = jnp.exp(-power * part)
    share = 1.0 / total
    rise = (expo - 1.0) / depth
    gap = 1.0 - bent
    sat = root * root
    conduct = ks * root * gap
    cond = conduct * gap
    dcond = conduct * rise * share * (0.5 * gap + 2.0 * bent * inverse)
    capacity = sat * (SPEC / STEP + (PORE / STEP) * rise * share)
    return cond, dcond, capacity


def couplings(k_own, dk_own, h_own, k_far, dk_far, h_far, tilt):
    part = 1.0 / (k_own + k_far)
    own, far = k_own * part, k_far * part
    slope = h_own - h_far - tilt
    near = 2.0 * far * (k_own + slope * far * dk_own)
    away = -2.0 * own * (k_far - slope * own * dk_far)
    return near, away


def lane_index(dims):
    return lax.broadcasted_iota(jnp.int32, dims, len(dims) - 1)


def row_index(dims):
    return lax.broadcasted_iota(jnp.int32, dims, len(dims) - 2)


def gather_sides(plane, z, odd_x, odd_y, packed):
    low, high = plane[0:1, :], plane[NX - 1 : NX, :]
    row_a = jnp.where(odd_x, low, high)
    row_b = jnp.where(odd_x, high, low)
    col_lane = lane_index((8, 128))
    left, right = plane[:, 0:128], plane[:, 128:256]
    for tile in range(TILES):
        first = jnp.broadcast_to(left[8 * tile : 8 * tile + 8, 0:1], (8, 128))
        last = jnp.broadcast_to(right[8 * tile : 8 * tile + 8, 127:128], (8, 128))
        col_a = jnp.where(odd_y, first, last)
        col_b = jnp.where(odd_y, last, first)
        packed = jnp.where(col_lane == TILES * z + tile, col_a, packed)
        packed = jnp.where(col_lane == TILES * z + tile + 64, col_b, packed)
    return row_a, row_b, packed


def spread_sides(z, odd_x, odd_y, rows_a, rows_b, packed):
    row = row_index((NX, NY))
    at_a = jnp.where(odd_x, 0, NX - 1)
    at_b = jnp.where(odd_x, NX - 1, 0)
    total = jnp.where(row == at_a, rows_a, 0.0) + jnp.where(row == at_b, rows_b, 0.0)
    turned = pltpu.roll(packed, 128 - TILES * z, axis=1)
    pieces = []
    lane = lane_index((8, 128))
    at_first = jnp.where(lane == 0, 1.0, 0.0)
    at_last = jnp.where(lane == 127, 1.0, 0.0)
    for tile in range(TILES):
        col_a = jnp.broadcast_to(turned[:, tile : tile + 1], (8, 128))
        col_b = jnp.broadcast_to(turned[:, tile + 64 : tile + 65], (8, 128))
        first = jnp.where(odd_y, col_a, col_b)
        last = jnp.where(odd_y, col_b, col_a)
        pieces.append(jnp.concatenate([first * at_first, last * at_last], axis=1))
    return total + jnp.concatenate(pieces, axis=0)


def odd_sides():
    return (lax.axis_index("gx_1") % 2) == 1, lax.axis_index("gy_1") == 1


def pack_kernel(head, soil, rhs, z_out, xa_out, xb_out, y_out):
    odd_x, odd_y = odd_sides()
    edge = jnp.where(lax.axis_index("gz") == 0, NZ - 1, 0)
    for slot, ref in enumerate((head, soil, rhs)):
        z_out[slot] = ref[edge].astype(F32)

        def plane_step(z, packed):
            row_a, row_b, packed = gather_sides(ref[z].astype(F32), z, odd_x, odd_y, packed)
            xa_out[slot, pl.ds(z, 1), :] = row_a
            xb_out[slot, pl.ds(z, 1), :] = row_b
            return packed

        y_out[slot] = lax.fori_loop(0, NZ, plane_step, jnp.zeros((8, 128), F32))


def terms_kernel(
    head, soil, rhs, xa, xb, y, alpha, expo, ks, coeffs, image, own_z, own_x, own_y, cond, dcond
):
    edge = jnp.where(lax.axis_index("gz") == 0, NZ - 1, 0)

    def terms_step(z, carry):
        k, dk, capacity = cell_terms(head[z], soil[z], alpha, expo, ks)
        cond[z], dcond[z], coeffs[0, z] = k, dk, capacity
        return carry

    lax.fori_loop(0, NZ, terms_step, 0)
    own_z[0], own_z[1] = cond[edge], dcond[edge]
    for slot, side in enumerate((xa, xb)):
        k, dk, _ = cell_terms(side[0], side[1].astype(jnp.int32), alpha, expo, ks)
        own_x[slot, 0], own_x[slot, 1] = k, dk
    k, dk, _ = cell_terms(y[0], y[1].astype(jnp.int32), alpha, expo, ks)
    own_y[0], own_y[1] = k, dk

    row, lane = row_index((NX, NY)), lane_index((NX, NY))

    def faces_step(z, carry):
        below_near, below_away = carry
        k, dk, h, v = cond[z], dcond[z], head[z], rhs[z]
        above = jnp.minimum(z + 1, NZ - 1)
        under = jnp.maximum(z - 1, 0)
        near, away = couplings(k, dk, h, cond[above], dcond[above], head[above], 1.0)
        inner = jnp.where(z < NZ - 1, 1.0, 0.0)
        near, away = near * inner, away * inner
        diagonal = coeffs[0, z] + near - below_away
        coeffs[1, z] = away
        coeffs[2, z] = -below_near
        total = away * rhs[above] - below_near * rhs[under]
        carry = near, away
        for slot, axis, position in ((3, 0, row), (5, 1, lane)):
            size = k.shape[axis]

            def up(x):
                return pltpu.roll(x, size - 1, axis=axis)

            def down(x):
                return pltpu.roll(x, 1, axis=axis)

            near, away = couplings(k, dk, h, up(k), up(dk), up(h), 0.0)
            inside = position < size - 1
            near, away = jnp.where(inside, near, 0.0), jnp.where(inside, away, 0.0)
            past = -down(near)
            diagonal = diagonal + near - down(away)
            coeffs[slot, z] = away
            coeffs[slot + 1, z] = past
            total = total + away * up(v) + past * down(v)
        coeffs[0, z] = diagonal
        image[z] = total + diagonal * v
        return carry

    nothing = jnp.zeros((NX, NY), F32)
    lax.fori_loop(0, NZ, faces_step, (nothing, nothing))


def pick_y(y_a, y_b):
    return jnp.where(lane_index(y_a.shape) < 64, y_a, y_b)


def first_kernel(
    head, boundary, rhs, interior, z_own, xa_own, xb_own, y_own, own_z, own_x, own_y,
    z_far, xa_far, xb_far, ya_far, yb_far, alpha, expo, ks,
    image, z_out, xa_out, xb_out, y_out, face_z, face_x, face_y,
):
    odd_x, odd_y = odd_sides()
    gz = lax.axis_index("gz")
    edge = jnp.where(gz == 0, NZ - 1, 0)
    tilt = jnp.where(gz == 0, 1.0, -1.0)
    gx, gy = along(GX), along(GY)
    has_x = jnp.logical_and(gx > 0, gx < lax.axis_size(GX) - 1)
    has_y = jnp.logical_and(gy > 0, gy < lax.axis_size(GY) - 1)

    def face(own, own_terms, far, there, slant):
        far_head = far[0] if there is None else jnp.where(there, far[0], -1.0)
        k, dk, _ = cell_terms(far_head, far[1].astype(jnp.int32), alpha, expo, ks)
        near, away = couplings(own_terms[0], own_terms[1], own[0], k, dk, far_head, slant)
        if there is not None:
            near, away = jnp.where(there, near, 0.0), jnp.where(there, away, 0.0)
        return near, away, near * own[2] + away * far[2]

    lane = lane_index((8, 128))
    far_y = tuple(pick_y(ya_far[slot], yb_far[slot]) for slot in range(3))
    there_y = jnp.logical_or(lane < 64, has_y)
    near, away, sum_y = face((y_own[0], None, y_own[2]), (own_y[0], own_y[1]), far_y, there_y, 0.0)
    face_y[0], face_y[1] = near, away
    sums_x = []
    for slot, (own, far, there) in enumerate(((xa_own, xa_far, None), (xb_own, xb_far, has_x))):
        near, away, total = face(own, (own_x[slot, 0], own_x[slot, 1]), far, there, 0.0)
        face_x[slot, 0], face_x[slot, 1] = near, away
        sums_x.append(total)
    near, away, sum_z = face(z_own, (own_z[0], own_z[1]), z_far, None, tilt)
    face_z[0], face_z[1] = near, away
    xa_out[...], xb_out[...] = sums_x
    image[...] = interior[...]
    image[edge] = image[edge] + sum_z

    def plane_step(z, packed):
        total = image[z] + spread_sides(
            z, odd_x, odd_y, xa_out[pl.ds(z, 1), :], xb_out[pl.ds(z, 1), :], sum_y
        )
        plane = jnp.where(boundary[z] == 1, rhs[z], total)
        image[z] = plane
        row_a, row_b, packed = gather_sides(plane, z, odd_x, odd_y, packed)
        xa_out[pl.ds(z, 1), :] = row_a
        xb_out[pl.ds(z, 1), :] = row_b
        return packed

    y_out[...] = lax.fori_loop(0, NZ, plane_step, jnp.zeros((8, 128), F32))
    z_out[...] = image[edge]


def fold(x):
    total = x[0:8, 0:128] + x[0:8, 128:256]
    for tile in range(1, TILES):
        total = total + x[8 * tile : 8 * tile + 8, 0:128] + x[8 * tile : 8 * tile + 8, 128:256]
    return total


def inner_kernel(coeffs, v_ref, rhs, interior, partial):
    def plane_step(z, sums):
        v, start = v_ref[z], rhs[z]
        above = jnp.minimum(z + 1, NZ - 1)
        under = jnp.maximum(z - 1, 0)
        total = coeffs[0, z] * v + coeffs[1, z] * v_ref[above] + coeffs[2, z] * v_ref[under]
        total = total + coeffs[3, z] * pltpu.roll(v, NX - 1, axis=0)
        total = total + coeffs[4, z] * pltpu.roll(v, 1, axis=0)
        total = total + coeffs[5, z] * pltpu.roll(v, NY - 1, axis=1)
        total = total + coeffs[6, z] * pltpu.roll(v, 1, axis=1)
        interior[z] = total
        products = (start * start, start * v, v * v)
        return tuple(s + fold(p) for s, p in zip(sums, products, strict=True))

    sums = lax.fori_loop(0, NZ, plane_step, (jnp.zeros((8, 128), F32),) * 3)
    for slot in range(3):
        partial[slot] = sums[slot]


def second_kernel(
    boundary, rhs, v_ref, interior, partial, z_own, xa_own, xb_own, y_own,
    z_far, xa_far, xb_far, ya_far, yb_far, face_z, face_x, face_y,
    image, sums_out, xa_sum, xb_sum,
):
    odd_x, odd_y = odd_sides()
    edge = jnp.where(lax.axis_index("gz") == 0, NZ - 1, 0)
    sum_y = face_y[0] * y_own[...] + face_y[1] * pick_y(ya_far[...], yb_far[...])
    xa_sum[...] = face_x[0, 0] * xa_own[...] + face_x[0, 1] * xa_far[...]
    xb_sum[...] = face_x[1, 0] * xb_own[...] + face_x[1, 1] * xb_far[...]
    image[...] = interior[...]
    image[edge] = image[edge] + face_z[0] * z_own[...] + face_z[1] * z_far[...]

    def plane_step(z, sums):
        v = v_ref[z]
        total = image[z] + spread_sides(
            z, odd_x, odd_y, xa_sum[pl.ds(z, 1), :], xb_sum[pl.ds(z, 1), :], sum_y
        )
        plane = jnp.where(boundary[z] == 1, v, total)
        image[z] = plane
        products = (plane * rhs[z], plane * v, plane * plane)
        return tuple(s + fold(p) for s, p in zip(sums, products, strict=True))

    sums = lax.fori_loop(0, NZ, plane_step, (jnp.zeros((8, 128), F32),) * 3)
    lane = lane_index((1, 8))
    row = jnp.zeros((1, 8), F32)
    for slot, part in enumerate((partial[0], partial[1], partial[2]) + sums):
        value = jnp.sum(jnp.sum(part, axis=0, keepdims=True), axis=1, keepdims=True)
        row = jnp.where(lane == slot, value, row)
    sums_out[...] = jnp.broadcast_to(row, sums_out.shape)


def least_squares(hess, beta):
    count = len(hess)
    rows = count + 1
    nothing = jnp.zeros_like(beta)
    columns = [[h[i] if i < len(h) else nothing for i in range(rows)] for h in hess]
    basis_q = []
    upper_r = [[None] * count for _ in range(count)]
    for column in range(count):
        vector = columns[column]
        for row in range(column):
            products = [q * c for q, c in zip(basis_q[row], columns[column], strict=True)]
            upper_r[row][column] = sum(products[1:], products[0])
        for row in range(column):
            scale = upper_r[row][column]
            vector = [v - scale * q for v, q in zip(vector, basis_q[row], strict=True)]
        squares = [v * v for v in vector]
        upper_r[column][column] = jnp.sqrt(sum(squares[1:], squares[0]))
        basis_q.append([v / upper_r[column][column] for v in vector])
    target = [beta * basis_q[row][0] for row in range(count)]
    solved = [None] * count
    for row in range(count - 1, -1, -1):
        value = target[row]
        for column in range(row + 1, count):
            value = value - upper_r[row][column] * solved[column]
        solved[row] = value / upper_r[row][row]
    return solved


def combine_kernel(rhs, first, second, sums, update, residual):
    total = jnp.sum(sums[...], axis=0, keepdims=True)
    g00, g01, g11, g02, g12, g22 = (total[:, i : i + 1] for i in range(6))
    square = g00 + EPS
    beta = jnp.sqrt(square)
    h00 = g01 / square
    rest = (g11 - 2.0 * h00 * g01 + h00 * h00 * g00) / square
    rest = jnp.maximum(rest, 0.0)
    h10 = jnp.sqrt(rest + EPS)
    h01 = (g02 - h00 * g01) / (square * h10)
    scale = square * h10 * h10
    h11 = (g12 - h00 * (g02 + g11 - h00 * g01)) / scale
    norm_w = (g22 - 2.0 * h00 * g12 + h00 * h00 * g11) / scale
    v00 = g00 / square
    v01 = (g01 - h00 * g00) / (square * h10)
    v11 = rest / (h10 * h10)
    last = norm_w - 2.0 * (h01 * h01 + h11 * h11)
    last = last + h01 * h01 * v00 + 2.0 * h01 * h11 * v01 + h11 * h11 * v11
    h21 = jnp.sqrt(jnp.maximum(last, 0.0) + EPS)
    y0, y1 = least_squares([[h00, h10], [h01, h11, h21]], beta)
    step = y1 / (beta * h10)
    base = y0 / beta - h00 * step

    def plane_step(z, carry):
        a, b, c = rhs[z], first[z], second[z]
        update[z] = base * a + step * b
        residual[z] = a - (base * b + step * c)
        return carry

    lax.fori_loop(0, NZ, plane_step, 0)


def cost(flops):
    return pl.CostEstimate(flops=flops, bytes_accessed=4 * 1024 * 1024, transcendentals=0)


def swap(x, axis, start, count):
    pairs = [(i, i + 1) for i in range(start, count - 1, 2)]
    return lax.ppermute(x, axis, pairs + [(b, a) for a, b in pairs])


def exchange(z, xa, xb, y):
    count_x, count_y = lax.axis_size(GX), lax.axis_size(GY)
    return (
        swap(z, "gz", 0, 2),
        swap(xa, GX, 0, count_x),
        swap(xb, GX, 1, count_x),
        swap(y, GY, 0, count_y),
        swap(y, GY, 1, count_y),
    )


def call(kernel, ins, outs, flops, scratch=()):
    return pl.pallas_call(
        kernel,
        out_shape=outs,
        in_specs=ins,
        out_specs=jax.tree.map(lambda _: VMEM, outs),
        scratch_shapes=list(scratch),
        compiler_params=PARAMS,
        cost_estimate=cost(flops),
        name=kernel.__name__,
    )


def body(head, soil, boundary, rhs, soil_alpha, soil_n, soil_ks):
    tables = (soil_alpha, soil_n, soil_ks)
    sides = (shape(3, NX, NY), shape(3, 8, NY), shape(3, 8, NY), shape(3, 8, 128))
    z, xa, xb, y = call(pack_kernel, [VMEM] * 3, sides, 1000000)(head, soil, rhs)
    far = exchange(z, xa, xb, y)
    own = (shape(2, NX, NY), shape(2, 2, 8, NY), shape(2, 8, 128))
    coeffs, interior, own_z, own_x, own_y = call(
        terms_kernel,
        [VMEM] * 6 + [SMEM] * 3,
        (shape(7, *BLOCK), shape(*BLOCK)) + own,
        40000000,
        (pltpu.VMEM(BLOCK, F32), pltpu.VMEM(BLOCK, F32)),
    )(head, soil, rhs, xa, xb, y, *tables)
    sides = (shape(NX, NY), shape(8, NY), shape(8, NY), shape(8, 128))
    first, z1, xa1, xb1, y1, face_z, face_x, face_y = call(
        first_kernel,
        [VMEM] * 16 + [SMEM] * 3,
        (shape(*BLOCK),) + sides + own,
        8000000,
    )(head, boundary, rhs, interior, z, xa, xb, y, own_z, own_x, own_y, *far, *tables)
    far = exchange(z1, xa1, xb1, y1)
    interior, partial = call(
        inner_kernel, [VMEM] * 3, (shape(*BLOCK), shape(3, 8, 128)), 8000000
    )(coeffs, first, rhs)
    second, sums = call(
        second_kernel,
        [VMEM] * 17,
        (shape(*BLOCK), shape(256, 8)),
        8000000,
        (pltpu.VMEM((8, NY), F32), pltpu.VMEM((8, NY), F32)),
    )(boundary, rhs, first, interior, partial, z1, xa1, xb1, y1, *far, face_z, face_x, face_y)
    sums = lax.all_to_all(sums, AXES, 0, 0)
    return call(combine_kernel, [VMEM] * 4, (shape(*BLOCK), shape(*BLOCK)), 1000000)(
        rhs, first, second, sums
    )


def solution(mesh):
    split = Mesh(mesh.devices.reshape(4, 4, 4, 2, mesh.shape["gz"]), AXES)
    in_specs = (P("gz", GX, GY),) * 4 + (P(), P(), P())
    out_specs = (P("gz", GX, GY), P("gz", GX, GY))
    return jax.shard_map(body, mesh=split, in_specs=in_specs, out_specs=out_specs, check_vma=False)
```

```python
import jax
import jax.numpy as jnp
from jax import lax
from jax.experimental import pallas as pl
from jax.experimental.pallas import tpu as pltpu
from jax.sharding import Mesh
from jax.sharding import PartitionSpec as P

AXES = ("gx_0", "gx_1", "gy_0", "gy_1", "gz")
GX = ("gx_0", "gx_1")
GY = ("gy_0", "gy_1")
SOILS = 8
EPS = 1e-06
SPEC = 0.0001
PORE = 0.4
STEP = 0.25
F32 = jnp.float32
NZ, NX, NY = 8, 64, 256
BLOCK = (NZ, NX, NY)
TILES = NX // 8
PARAMS = pltpu.CompilerParams(vmem_limit_bytes=24 * 1024 * 1024)
VMEM = pl.BlockSpec(memory_space=pltpu.VMEM)
HBM = pl.BlockSpec(memory_space=pltpu.HBM)


def shape(*dims):
    return jax.ShapeDtypeStruct(dims, F32)


def along(axes):
    index = lax.axis_index(axes[0])
    return index * lax.axis_size(axes[1]) + lax.axis_index(axes[1])


def cell_terms(head, soil, tables):
    def entry_of(table, entry):
        line = tables[table, entry : entry + 1, :]
        if head.shape[1] == 256:
            line = jnp.concatenate([line, line], axis=1)
        return jnp.broadcast_to(line, head.shape)

    picked = [entry_of(table, 0) for table in range(4)]
    for entry in range(1, SOILS):
        here = soil == entry
        picked = [jnp.where(here, entry_of(t, entry), x) for t, x in enumerate(picked)]
    alpha, expo, ks, power = picked
    depth = -head
    scaled = expo * jnp.log(alpha * depth)
    inverse = jnp.exp(-scaled)
    total = 1.0 + inverse
    part = jnp.log(total)
    root = jnp.exp((-0.5 * power) * (part + scaled))
    bent = jnp.exp(-power * part)
    share = 1.0 / total
    rise = (expo - 1.0) / depth
    gap = 1.0 - bent
    sat = root * root
    conduct = ks * root * gap
    cond = conduct * gap
    dcond = conduct * rise * share * (0.5 * gap + 2.0 * bent * inverse)
    capacity = sat * (SPEC / STEP + (PORE / STEP) * rise * share)
    return cond, dcond, capacity


def couplings(k_own, dk_own, h_own, k_far, dk_far, h_far, tilt):
    part = 1.0 / (k_own + k_far)
    own, far = k_own * part, k_far * part
    slope = h_own - h_far - tilt
    near = 2.0 * far * (k_own + slope * far * dk_own)
    away = -2.0 * own * (k_far - slope * own * dk_far)
    return near, away


def lane_index(dims):
    return lax.broadcasted_iota(jnp.int32, dims, len(dims) - 1)


def row_index(dims):
    return lax.broadcasted_iota(jnp.int32, dims, len(dims) - 2)


def gather_columns(plane, z, first_at, last_at, packed):
    lane = lane_index((8, 128))
    for tile in range(TILES):
        rows = slice(8 * tile, 8 * tile + 8)
        first = jnp.broadcast_to(plane[rows, 0:1], (8, 128))
        last = jnp.broadcast_to(plane[rows, NY - 1 : NY], (8, 128))
        packed = jnp.where(lane == TILES * z + tile + first_at, first, packed)
        packed = jnp.where(lane == TILES * z + tile + last_at, last, packed)
    return packed


def gather_rows(plane, odd_x):
    low, high = plane[0:1, :], plane[NX - 1 : NX, :]
    return jnp.where(odd_x, low, high), jnp.where(odd_x, high, low)


def spread_sides(z, odd_x, odd_y, row_a, row_b, packed):
    low, high = jnp.where(odd_x, row_a, row_b), jnp.where(odd_x, row_b, row_a)
    first = jnp.where(odd_y, packed, pltpu.roll(packed, 64, axis=1))
    lane, row = lane_index((8, 128)), row_index((8, NY))
    pieces = []
    for tile in range(TILES):
        at = TILES * z + tile
        left = jnp.broadcast_to(first[:, at : at + 1], (8, 128))
        right = jnp.broadcast_to(first[:, at + 64 : at + 65], (8, 128))
        left, right = jnp.where(lane == 0, left, 0.0), jnp.where(lane == 127, right, 0.0)
        piece = jnp.concatenate([left, right], axis=1)
        if tile == 0:
            piece = piece + jnp.where(row == 0, low, 0.0)
        if tile == TILES - 1:
            piece = piece + jnp.where(row == 7, high, 0.0)
        pieces.append(piece)
    return jnp.concatenate(pieces, axis=0)


def odd_sides():
    return (lax.axis_index("gx_1") % 2) == 1, lax.axis_index("gy_1") == 1


def column_lanes(odd_y):
    return jnp.where(odd_y, 0, 64), jnp.where(odd_y, 64, 0)


def pack_kernel(
    head, soil, boundary, rhs, alpha, expo, ks,
    head_out, soil_out, boundary_out, rhs_out, tables, z_out, xa_out, xb_out, y_out,
    alpha_in, expo_in, ks_in, arrived,
):
    pairs = (
        (alpha, alpha_in), (expo, expo_in), (ks, ks_in),
        (head, head_out), (soil, soil_out), (rhs, rhs_out), (boundary, boundary_out),
    )
    copies = [
        pltpu.make_async_copy(source, target, arrived.at[i])
        for i, (source, target) in enumerate(pairs)
    ]
    for copy in copies:
        copy.start()
    odd_x, odd_y = odd_sides()
    edge = jnp.where(lax.axis_index("gz") == 0, NZ - 1, 0)
    first_at, last_at = column_lanes(odd_y)
    row = row_index((8, 128))
    lines = []
    for copy, source in zip(copies[:3], (alpha_in, expo_in, ks_in), strict=True):
        copy.wait()
        line = jnp.full((8, 128), source[0], F32)
        for entry in range(1, SOILS):
            line = jnp.where(row == entry, source[entry], line)
        lines.append(line)
    for slot, line in enumerate(lines + [1.0 - 1.0 / lines[1]]):
        tables[slot] = line
    for slot, (copy, ref) in enumerate(
        zip(copies[3:6], (head_out, soil_out, rhs_out), strict=True)
    ):
        copy.wait()
        z_out[slot] = ref[edge].astype(F32)
        packed = jnp.zeros((8, 128), F32)
        for z in range(NZ):
            plane = ref[z].astype(F32)
            packed = gather_columns(plane, z, first_at, last_at, packed)
            row_a, row_b = gather_rows(plane, odd_x)
            xa_out[slot, z : z + 1, :] = row_a
            xb_out[slot, z : z + 1, :] = row_b
        y_out[slot] = packed
    copies[6].wait()


def terms_kernel(
    head, soil, rhs, xa, xb, y, tables, coeffs, image, own_z, own_x, own_y, cond, dcond
):
    edge = jnp.where(lax.axis_index("gz") == 0, NZ - 1, 0)

    def terms_step(z, carry):
        k, dk, capacity = cell_terms(head[z], soil[z], tables)
        cond[z], dcond[z], coeffs[0, z] = k, dk, capacity
        return carry

    lax.fori_loop(0, NZ, terms_step, 0)
    own_z[0], own_z[1] = cond[edge], dcond[edge]
    for slot, side in enumerate((xa, xb)):
        k, dk, _ = cell_terms(side[0], side[1].astype(jnp.int32), tables)
        own_x[slot, 0], own_x[slot, 1] = k, dk
    k, dk, _ = cell_terms(y[0], y[1].astype(jnp.int32), tables)
    own_y[0], own_y[1] = k, dk

    row, lane = row_index((NX, NY)), lane_index((NX, NY))

    def faces_step(z, carry):
        below_near, below_away = carry
        k, dk, h, v = cond[z], dcond[z], head[z], rhs[z]
        above = jnp.minimum(z + 1, NZ - 1)
        under = jnp.maximum(z - 1, 0)
        near, away = couplings(k, dk, h, cond[above], dcond[above], head[above], 1.0)
        inner = jnp.where(z < NZ - 1, 1.0, 0.0)
        near, away = near * inner, away * inner
        diagonal = coeffs[0, z] + near - below_away
        coeffs[1, z] = away
        coeffs[2, z] = -below_near
        total = away * rhs[above] - below_near * rhs[under]
        carry = near, away
        for slot, axis, position in ((3, 0, row), (5, 1, lane)):
            size = k.shape[axis]

            def up(x):
                return pltpu.roll(x, size - 1, axis=axis)

            def down(x):
                return pltpu.roll(x, 1, axis=axis)

            near, away = couplings(k, dk, h, up(k), up(dk), up(h), 0.0)
            inside = position < size - 1
            near, away = jnp.where(inside, near, 0.0), jnp.where(inside, away, 0.0)
            past = -down(near)
            diagonal = diagonal + near - down(away)
            coeffs[slot, z] = away
            coeffs[slot + 1, z] = past
            total = total + away * up(v) + past * down(v)
        coeffs[0, z] = diagonal
        image[z] = total + diagonal * v
        return carry

    nothing = jnp.zeros((NX, NY), F32)
    lax.fori_loop(0, NZ, faces_step, (nothing, nothing))


def pick_y(y_a, y_b):
    return jnp.where(lane_index(y_a.shape) < 64, y_a, y_b)


def first_kernel(
    head, boundary, rhs, interior, z_own, xa_own, xb_own, y_own, own_z, own_x, own_y,
    z_far, xa_far, xb_far, ya_far, yb_far, tables,
    image, z_out, xa_out, xb_out, y_out, face_z, face_x, face_y,
):
    odd_x, odd_y = odd_sides()
    gz = lax.axis_index("gz")
    edge = jnp.where(gz == 0, NZ - 1, 0)
    tilt = jnp.where(gz == 0, 1.0, -1.0)
    gx, gy = along(GX), along(GY)
    has_x = jnp.logical_and(gx > 0, gx < lax.axis_size(GX) - 1)
    has_y = jnp.logical_and(gy > 0, gy < lax.axis_size(GY) - 1)

    def face(own, own_terms, far, there, slant):
        far_head = far[0] if there is None else jnp.where(there, far[0], -1.0)
        k, dk, _ = cell_terms(far_head, far[1].astype(jnp.int32), tables)
        near, away = couplings(own_terms[0], own_terms[1], own[0], k, dk, far_head, slant)
        if there is not None:
            near, away = jnp.where(there, near, 0.0), jnp.where(there, away, 0.0)
        return near, away, near * own[2] + away * far[2]

    lane = lane_index((8, 128))
    far_y = tuple(pick_y(ya_far[slot], yb_far[slot]) for slot in range(3))
    there_y = jnp.logical_or(lane < 64, has_y)
    near, away, sum_y = face((y_own[0], None, y_own[2]), (own_y[0], own_y[1]), far_y, there_y, 0.0)
    face_y[0], face_y[1] = near, away
    sums_x = []
    for slot, (own, far, there) in enumerate(((xa_own, xa_far, None), (xb_own, xb_far, has_x))):
        near, away, total = face(own, (own_x[slot, 0], own_x[slot, 1]), far, there, 0.0)
        face_x[slot, 0], face_x[slot, 1] = near, away
        sums_x.append(total)
    near, away, sum_z = face(z_own, (own_z[0], own_z[1]), z_far, None, tilt)
    face_z[0], face_z[1] = near, away
    image[...] = interior[...]
    image[edge] = image[edge] + sum_z

    first_at, last_at = column_lanes(odd_y)
    packed = jnp.zeros((8, 128), F32)
    for z in range(NZ):
        total = image[z] + spread_sides(
            z, odd_x, odd_y, sums_x[0][z : z + 1, :], sums_x[1][z : z + 1, :], sum_y
        )
        plane = jnp.where(boundary[z] == 1, rhs[z], total)
        image[z] = plane
        row_a, row_b = gather_rows(plane, odd_x)
        xa_out[z : z + 1, :] = row_a
        xb_out[z : z + 1, :] = row_b
        packed = gather_columns(plane, z, first_at, last_at, packed)
    y_out[...] = packed
    z_out[...] = image[edge]


def fold(x):
    total = x[0:8, 0:128] + x[0:8, 128:256]
    for tile in range(1, TILES):
        total = total + x[8 * tile : 8 * tile + 8, 0:128] + x[8 * tile : 8 * tile + 8, 128:256]
    return total


def inner_kernel(coeffs, v_ref, rhs, interior, partial):
    def plane_step(z, sums):
        v, start = v_ref[z], rhs[z]
        above = jnp.minimum(z + 1, NZ - 1)
        under = jnp.maximum(z - 1, 0)
        total = coeffs[0, z] * v + coeffs[1, z] * v_ref[above] + coeffs[2, z] * v_ref[under]
        total = total + coeffs[3, z] * pltpu.roll(v, NX - 1, axis=0)
        total = total + coeffs[4, z] * pltpu.roll(v, 1, axis=0)
        total = total + coeffs[5, z] * pltpu.roll(v, NY - 1, axis=1)
        total = total + coeffs[6, z] * pltpu.roll(v, 1, axis=1)
        interior[z] = total
        products = (start * start, start * v, v * v)
        return tuple(s + fold(p) for s, p in zip(sums, products, strict=True))

    sums = lax.fori_loop(0, NZ, plane_step, (jnp.zeros((8, 128), F32),) * 3)
    for slot in range(3):
        partial[slot] = sums[slot]


def second_kernel(
    boundary, rhs, v_ref, interior, partial, z_own, xa_own, xb_own, y_own,
    z_far, xa_far, xb_far, ya_far, yb_far, face_z, face_x, face_y,
    image, sums_out,
):
    odd_x, odd_y = odd_sides()
    edge = jnp.where(lax.axis_index("gz") == 0, NZ - 1, 0)
    sum_y = face_y[0] * y_own[...] + face_y[1] * pick_y(ya_far[...], yb_far[...])
    sum_xa = face_x[0, 0] * xa_own[...] + face_x[0, 1] * xa_far[...]
    sum_xb = face_x[1, 0] * xb_own[...] + face_x[1, 1] * xb_far[...]
    image[...] = interior[...]
    image[edge] = image[edge] + face_z[0] * z_own[...] + face_z[1] * z_far[...]

    sums = None
    for z in range(NZ):
        v = v_ref[z]
        total = image[z] + spread_sides(
            z, odd_x, odd_y, sum_xa[z : z + 1, :], sum_xb[z : z + 1, :], sum_y
        )
        plane = jnp.where(boundary[z] == 1, v, total)
        image[z] = plane
        products = [fold(p) for p in (plane * rhs[z], plane * v, plane * plane)]
        sums = products if z == 0 else [s + p for s, p in zip(sums, products, strict=True)]
    lane = lane_index((1, 8))
    row = jnp.zeros((1, 8), F32)
    for slot, part in enumerate([partial[0], partial[1], partial[2]] + sums):
        value = jnp.sum(jnp.sum(part, axis=0, keepdims=True), axis=1, keepdims=True)
        row = jnp.where(lane == slot, value, row)
    sums_out[...] = jnp.broadcast_to(row, sums_out.shape)


def least_squares(hess, beta):
    count = len(hess)
    rows = count + 1
    nothing = jnp.zeros_like(beta)
    columns = [[h[i] if i < len(h) else nothing for i in range(rows)] for h in hess]
    basis_q = []
    upper_r = [[None] * count for _ in range(count)]
    for column in range(count):
        vector = columns[column]
        for row in range(column):
            products = [q * c for q, c in zip(basis_q[row], columns[column], strict=True)]
            upper_r[row][column] = sum(products[1:], products[0])
        for row in range(column):
            scale = upper_r[row][column]
            vector = [v - scale * q for v, q in zip(vector, basis_q[row], strict=True)]
        squares = [v * v for v in vector]
        upper_r[column][column] = jnp.sqrt(sum(squares[1:], squares[0]))
        basis_q.append([v / upper_r[column][column] for v in vector])
    target = [beta * basis_q[row][0] for row in range(count)]
    solved = [None] * count
    for row in range(count - 1, -1, -1):
        value = target[row]
        for column in range(row + 1, count):
            value = value - upper_r[row][column] * solved[column]
        solved[row] = value / upper_r[row][row]
    return solved


def combine_kernel(rhs, first, second, sums, update_out, residual_out, update, residual, left):
    total = jnp.sum(sums[...], axis=0, keepdims=True)
    g00, g01, g11, g02, g12, g22 = (total[:, i : i + 1] for i in range(6))
    square = g00 + EPS
    beta = jnp.sqrt(square)
    h00 = g01 / square
    rest = (g11 - 2.0 * h00 * g01 + h00 * h00 * g00) / square
    rest = jnp.maximum(rest, 0.0)
    h10 = jnp.sqrt(rest + EPS)
    h01 = (g02 - h00 * g01) / (square * h10)
    scale = square * h10 * h10
    h11 = (g12 - h00 * (g02 + g11 - h00 * g01)) / scale
    norm_w = (g22 - 2.0 * h00 * g12 + h00 * h00 * g11) / scale
    v00 = g00 / square
    v01 = (g01 - h00 * g00) / (square * h10)
    v11 = rest / (h10 * h10)
    last = norm_w - 2.0 * (h01 * h01 + h11 * h11)
    last = last + h01 * h01 * v00 + 2.0 * h01 * h11 * v01 + h11 * h11 * v11
    h21 = jnp.sqrt(jnp.maximum(last, 0.0) + EPS)
    y0, y1 = least_squares([[h00, h10], [h01, h11, h21]], beta)
    step = y1 / (beta * h10)
    base = y0 / beta - h00 * step

    def plane_step(z, carry):
        a, b, c = rhs[z], first[z], second[z]
        update[z] = base * a + step * b
        residual[z] = a - (base * b + step * c)
        for slot, (source, target) in enumerate(pairs):
            pltpu.make_async_copy(source.at[z], target.at[z], left.at[slot, z]).start()
        return carry

    pairs = ((update, update_out), (residual, residual_out))
    lax.fori_loop(0, NZ, plane_step, 0)
    for z in range(NZ):
        for slot, (source, target) in enumerate(pairs):
            pltpu.make_async_copy(source.at[z], target.at[z], left.at[slot, z]).wait()


def cost(flops):
    return pl.CostEstimate(flops=flops, bytes_accessed=4 * 1024 * 1024, transcendentals=0)


def swap(x, axis, start, count):
    pairs = [(i, (i + 1) % count) for i in range(start, count, 2)]
    return lax.ppermute(x, axis, pairs + [(b, a) for a, b in pairs])


def exchange(z, xa, xb, y):
    count_x, count_y = lax.axis_size(GX), lax.axis_size(GY)
    return (
        swap(z, "gz", 0, 2),
        swap(xa, GX, 0, count_x),
        swap(xb, GX, 1, count_x),
        swap(y, GY, 0, count_y),
        swap(y, GY, 1, count_y),
    )


def call(kernel, ins, outs, flops, out_specs=None, scratch=()):
    return pl.pallas_call(
        kernel,
        out_shape=outs,
        in_specs=ins,
        out_specs=out_specs or tuple(VMEM for _ in outs),
        scratch_shapes=list(scratch),
        compiler_params=PARAMS,
        cost_estimate=cost(flops),
        name=kernel.__name__,
    )


def body(head, soil, boundary, rhs, soil_alpha, soil_n, soil_ks):
    whole = shape(*BLOCK)
    counts = jax.ShapeDtypeStruct(BLOCK, jnp.int32)
    sides = (shape(3, NX, NY), shape(3, 8, NY), shape(3, 8, NY), shape(3, 8, 128))
    sources = (head, soil, boundary, rhs, soil_alpha, soil_n, soil_ks)
    sources = [pltpu.with_memory_space_constraint(x, pltpu.HBM) for x in sources]
    head, soil, boundary, rhs, tables, z, xa, xb, y = call(
        pack_kernel,
        [HBM] * 7,
        (whole, counts, counts, whole, shape(4, 8, 128)) + sides,
        1000000,
        scratch=[pltpu.SMEM((SOILS,), F32)] * 3 + [pltpu.SemaphoreType.DMA((7,))],
    )(*sources)
    far = exchange(z, xa, xb, y)
    own = (shape(2, NX, NY), shape(2, 2, 8, NY), shape(2, 8, 128))
    coeffs, interior, own_z, own_x, own_y = call(
        terms_kernel,
        [VMEM] * 7,
        (shape(7, *BLOCK), whole) + own,
        40000000,
        scratch=[pltpu.VMEM(BLOCK, F32)] * 2,
    )(head, soil, rhs, xa, xb, y, tables)
    sides = (shape(NX, NY), shape(8, NY), shape(8, NY), shape(8, 128))
    first, z1, xa1, xb1, y1, face_z, face_x, face_y = call(
        first_kernel, [VMEM] * 17, (whole,) + sides + own, 8000000
    )(head, boundary, rhs, interior, z, xa, xb, y, own_z, own_x, own_y, *far, tables)
    far = exchange(z1, xa1, xb1, y1)
    interior, partial = call(inner_kernel, [VMEM] * 3, (whole, shape(3, 8, 128)), 8000000)(
        coeffs, first, rhs
    )
    second, sums = call(second_kernel, [VMEM] * 17, (whole, shape(256, 8)), 8000000)(
        boundary, rhs, first, interior, partial, z1, xa1, xb1, y1, *far, face_z, face_x, face_y
    )
    sums = lax.all_to_all(sums, AXES, 0, 0)
    return call(
        combine_kernel,
        [VMEM] * 4,
        (whole, whole),
        1000000,
        (HBM, HBM),
        [pltpu.VMEM(BLOCK, F32)] * 2 + [pltpu.SemaphoreType.DMA((2, NZ))],
    )(rhs, first, second, sums)


def solution(mesh):
    split = Mesh(mesh.devices.reshape(4, 4, 4, 2, mesh.shape["gz"]), AXES)
    in_specs = (P("gz", GX, GY),) * 4 + (P(), P(), P())
    out_specs = (P("gz", GX, GY), P("gz", GX, GY))
    return jax.shard_map(body, mesh=split, in_specs=in_specs, out_specs=out_specs, check_vma=False)
```

```python
import jax
import jax.numpy as jnp
from jax import lax
from jax.experimental import pallas as pl
from jax.experimental.pallas import tpu as pltpu
from jax.sharding import Mesh
from jax.sharding import PartitionSpec as P


AXES = ("gx_0", "gx_1", "gy_0", "gy_1", "gz")
GX = ("gx_0", "gx_1")
GY = ("gy_0", "gy_1")
SOILS = 8
EPS = 1e-06
SPEC = 0.0001
PORE = 0.4
STEP = 0.25
F32 = jnp.float32
LOG2E = 1.4426950408889634
NZ, NX, NY = 8, 64, 256
BLOCK = (NZ, NX, NY)
TILES = NX // 8
PARAMS = pltpu.CompilerParams(vmem_limit_bytes=24 * 1024 * 1024)
VMEM = pl.BlockSpec(memory_space=pltpu.VMEM)
HBM = pl.BlockSpec(memory_space=pltpu.HBM)


def shape(*dims):
    return jax.ShapeDtypeStruct(dims, F32)


def along(axes):
    index = lax.axis_index(axes[0])
    return index * lax.axis_size(axes[1]) + lax.axis_index(axes[1])


def pick(tables, soil):
    rows = []
    for row in range(0, soil.shape[0], 8):
        tiles = []
        for lane in range(0, soil.shape[1], 128):
            index = soil[row : row + 8, lane : lane + 128]
            tiles.append(
                [
                    jnp.take_along_axis(tables[t], index, axis=0, mode="promise_in_bounds")
                    for t in range(4)
                ]
            )
        rows.append([jnp.concatenate(x, axis=1) for x in zip(*tiles, strict=True)])
    return [jnp.concatenate(x, axis=0) for x in zip(*rows, strict=True)]


def cell_terms(head, soil, tables):
    minus_alpha, expo, ks, minus_power = pick(tables, soil)
    scaled = expo * jnp.log(minus_alpha * head)
    inverse = jnp.exp2(-LOG2E * scaled)
    total = 1.0 + inverse
    part = jnp.log(total)
    root = jnp.exp2(0.5 * (minus_power * (part + scaled)))
    bent = jnp.exp2(minus_power * part)
    rise = (1.0 - expo) / (head * total)
    gap = 1.0 - bent
    conduct = ks * root * gap
    cond = 2.0 * (conduct * gap)
    dcond = conduct * rise * (gap + 4.0 * (bent * inverse))
    capacity = root * root * (SPEC / STEP + (PORE / STEP) * rise)
    return cond, dcond, capacity


def couplings(k_own, dk_own, h_own, k_far, dk_far, h_far, tilt):
    part = 1.0 / (k_own + k_far)
    own, far = k_own * part, k_far * part
    slope = h_own - h_far
    if tilt is not None:
        slope = slope - tilt
    mean = far * k_own
    near = mean + far * far * (slope * dk_own)
    away = own * own * (slope * dk_far) - mean
    return near, away


def lane_index(dims):
    return lax.broadcasted_iota(jnp.int32, dims, len(dims) - 1)


def row_index(dims):
    return lax.broadcasted_iota(jnp.int32, dims, len(dims) - 2)


def gather_columns(plane, z, first_at, last_at, packed):
    lane = lane_index((8, 128))
    for tile in range(TILES):
        rows = slice(8 * tile, 8 * tile + 8)
        first = jnp.broadcast_to(plane[rows, 0:1], (8, 128))
        last = jnp.broadcast_to(plane[rows, NY - 1 : NY], (8, 128))
        packed = jnp.where(lane == TILES * z + tile + first_at, first, packed)
        packed = jnp.where(lane == TILES * z + tile + last_at, last, packed)
    return packed


def gather_rows(plane, odd_x):
    low, high = plane[0:1, :], plane[NX - 1 : NX, :]
    return jnp.where(odd_x, low, high), jnp.where(odd_x, high, low)


def spread_sides(z, odd_x, odd_y, row_a, row_b, packed):
    low, high = jnp.where(odd_x, row_a, row_b), jnp.where(odd_x, row_b, row_a)
    first = jnp.where(odd_y, packed, pltpu.roll(packed, 64, axis=1))
    lane, row = lane_index((8, 128)), row_index((8, NY))
    pieces = []
    for tile in range(TILES):
        at = TILES * z + tile
        left = jnp.broadcast_to(first[:, at : at + 1], (8, 128))
        right = jnp.broadcast_to(first[:, at + 64 : at + 65], (8, 128))
        left, right = jnp.where(lane == 0, left, 0.0), jnp.where(lane == 127, right, 0.0)
        piece = jnp.concatenate([left, right], axis=1)
        if tile == 0:
            piece = piece + jnp.where(row == 0, low, 0.0)
        if tile == TILES - 1:
            piece = piece + jnp.where(row == 7, high, 0.0)
        pieces.append(piece)
    return jnp.concatenate(pieces, axis=0)


def odd_sides():
    return (lax.axis_index("gx_1") % 2) == 1, lax.axis_index("gy_1") == 1


def column_lanes(odd_y):
    return jnp.where(odd_y, 0, 64), jnp.where(odd_y, 64, 0)


def pack_kernel(
    head, soil, rhs, alpha, expo, ks,
    head_out, soil_out, rhs_out, tables, z_out, xa_out, xb_out, y_out,
    alpha_in, expo_in, ks_in, arrived,
):
    pairs = (
        (alpha, alpha_in), (expo, expo_in), (ks, ks_in),
        (head, head_out), (soil, soil_out), (rhs, rhs_out),
    )
    copies = [
        pltpu.make_async_copy(source, target, arrived.at[i])
        for i, (source, target) in enumerate(pairs)
    ]
    for copy in copies:
        copy.start()
    odd_x, odd_y = odd_sides()
    edge = jnp.where(lax.axis_index("gz") == 0, NZ - 1, 0)
    first_at, last_at = column_lanes(odd_y)
    row = row_index((8, 128))
    lines = []
    for copy, source in zip(copies[:3], (alpha_in, expo_in, ks_in), strict=True):
        copy.wait()
        line = jnp.full((8, 128), source[0], F32)
        for entry in range(1, SOILS):
            line = jnp.where(row == entry, source[entry], line)
        lines.append(line)
    lines[0] = -lines[0]
    for slot, line in enumerate(lines + [LOG2E / lines[1] - LOG2E]):
        tables[slot] = line
    for slot, (copy, ref) in enumerate(
        zip(copies[3:6], (head_out, soil_out, rhs_out), strict=True)
    ):
        copy.wait()
        z_out[slot] = ref[edge].astype(F32)
        packed = jnp.zeros((8, 128), F32)
        for z in range(NZ):
            plane = ref[z].astype(F32)
            packed = gather_columns(plane, z, first_at, last_at, packed)
            row_a, row_b = gather_rows(plane, odd_x)
            xa_out[slot, z : z + 1, :] = row_a
            xb_out[slot, z : z + 1, :] = row_b
        y_out[slot] = packed


def end_rows(x):
    tail = x[NX - 8 :, :]
    tail = jnp.where(row_index(tail.shape) < 7, tail, 0.0)
    return jnp.concatenate([x[: NX - 8, :], tail], axis=0)


def end_lanes(x):
    tail = x[:, NY - 128 :]
    tail = jnp.where(lane_index(tail.shape) < 127, tail, 0.0)
    return jnp.concatenate([x[:, : NY - 128], tail], axis=1)


def up(x, axis):
    return pltpu.roll(x, x.shape[axis] - 1, axis=axis)


def terms_kernel(
    head, soil, rhs, xa, xb, y, tables, boundary,
    coeffs, image, own_z, own_x, own_y, boundary_out, cond, dcond, arrived,
):
    copy = pltpu.make_async_copy(boundary, boundary_out, arrived)
    copy.start()
    edge = jnp.where(lax.axis_index("gz") == 0, NZ - 1, 0)

    def terms_step(z, carry):
        k, dk, capacity = cell_terms(head[z], soil[z], tables)
        cond[z], dcond[z], coeffs[0, z] = k, dk, capacity
        return carry

    lax.fori_loop(0, NZ, terms_step, 0)
    nothing = jnp.zeros((NX, NY), F32)
    cond[NZ], dcond[NZ] = nothing, nothing
    own_z[0], own_z[1] = cond[edge], dcond[edge]
    for slot, side in enumerate((xa, xb)):
        k, dk, _ = cell_terms(side[0], side[1].astype(jnp.int32), tables)
        own_x[slot, 0], own_x[slot, 1] = k, dk
    k, dk, _ = cell_terms(y[0], y[1].astype(jnp.int32), tables)
    own_y[0], own_y[1] = k, dk

    def faces_step(z, below):
        k, dk, h, v = cond[z], dcond[z], head[z], rhs[z]
        above = jnp.minimum(z + 1, NZ - 1)
        near, away = couplings(k, dk, h, cond[z + 1], dcond[z + 1], head[above], 1.0)
        coeffs[1, z], coeffs[2, z] = near, away
        flux = near * v + away * rhs[above]
        total = coeffs[0, z] * v + flux - below
        below = flux
        for slot, axis, end in ((3, 0, end_rows), (5, 1, end_lanes)):
            far = (end(up(k, axis)), end(up(dk, axis)), up(h, axis))
            near, away = couplings(k, dk, h, *far, None)
            coeffs[slot, z], coeffs[slot + 1, z] = near, away
            flux = near * v + away * up(v, axis)
            total = total + flux - pltpu.roll(flux, 1, axis=axis)
        image[z] = total
        return below

    lax.fori_loop(0, NZ, faces_step, nothing)
    copy.wait()


def pick_y(y_a, y_b):
    return jnp.where(lane_index(y_a.shape) < 64, y_a, y_b)


def first_kernel(
    head, boundary, rhs, interior, z_own, xa_own, xb_own, y_own, own_z, own_x, own_y,
    z_far, xa_far, xb_far, ya_far, yb_far, tables,
    image, z_out, xa_out, xb_out, y_out, face_z, face_x, face_y,
):
    odd_x, odd_y = odd_sides()
    gz = lax.axis_index("gz")
    edge = jnp.where(gz == 0, NZ - 1, 0)
    tilt = jnp.where(gz == 0, 1.0, -1.0)
    gx, gy = along(GX), along(GY)
    has_x = jnp.logical_and(gx > 0, gx < lax.axis_size(GX) - 1)
    has_y = jnp.logical_and(gy > 0, gy < lax.axis_size(GY) - 1)

    def face(own, own_terms, far, there, slant):
        far_head = far[0] if there is None else jnp.where(there, far[0], -1.0)
        k, dk, _ = cell_terms(far_head, far[1].astype(jnp.int32), tables)
        near, away = couplings(own_terms[0], own_terms[1], own[0], k, dk, far_head, slant)
        if there is not None:
            near, away = jnp.where(there, near, 0.0), jnp.where(there, away, 0.0)
        return near, away, near * own[2] + away * far[2]

    lane = lane_index((8, 128))
    far_y = tuple(pick_y(ya_far[slot], yb_far[slot]) for slot in range(3))
    there_y = jnp.logical_or(lane < 64, has_y)
    near, away, sum_y = face((y_own[0], None, y_own[2]), (own_y[0], own_y[1]), far_y, there_y, None)
    face_y[0], face_y[1] = near, away
    sums_x = []
    for slot, (own, far, there) in enumerate(((xa_own, xa_far, None), (xb_own, xb_far, has_x))):
        near, away, total = face(own, (own_x[slot, 0], own_x[slot, 1]), far, there, None)
        face_x[slot, 0], face_x[slot, 1] = near, away
        sums_x.append(total)
    near, away, sum_z = face(z_own, (own_z[0], own_z[1]), z_far, None, tilt)
    face_z[0], face_z[1] = near, away
    image[...] = interior[...]
    image[edge] = image[edge] + sum_z

    first_at, last_at = column_lanes(odd_y)
    packed = jnp.zeros((8, 128), F32)
    for z in range(NZ):
        total = image[z] + spread_sides(
            z, odd_x, odd_y, sums_x[0][z : z + 1, :], sums_x[1][z : z + 1, :], sum_y
        )
        plane = jnp.where(boundary[z] == 1, rhs[z], total)
        image[z] = plane
        row_a, row_b = gather_rows(plane, odd_x)
        xa_out[z : z + 1, :] = row_a
        xb_out[z : z + 1, :] = row_b
        packed = gather_columns(plane, z, first_at, last_at, packed)
    y_out[...] = packed
    z_out[...] = image[edge]


def fold(x):
    total = x[0:8, 0:128] + x[0:8, 128:256]
    for tile in range(1, TILES):
        total = total + x[8 * tile : 8 * tile + 8, 0:128] + x[8 * tile : 8 * tile + 8, 128:256]
    return total


def inner_kernel(coeffs, v_ref, rhs, interior, partial):
    def plane_step(z, carry):
        below, sums = carry
        v, start = v_ref[z], rhs[z]
        above = jnp.minimum(z + 1, NZ - 1)
        flux = coeffs[1, z] * v + coeffs[2, z] * v_ref[above]
        total = coeffs[0, z] * v + flux - below
        below = flux
        for slot, axis in ((3, 0), (5, 1)):
            flux = coeffs[slot, z] * v + coeffs[slot + 1, z] * up(v, axis)
            total = total + flux - pltpu.roll(flux, 1, axis=axis)
        interior[z] = total
        products = (start * start, start * v, v * v)
        return below, tuple(s + fold(p) for s, p in zip(sums, products, strict=True))

    carry = jnp.zeros((NX, NY), F32), (jnp.zeros((8, 128), F32),) * 3
    _, sums = lax.fori_loop(0, NZ, plane_step, carry)
    for slot in range(3):
        partial[slot] = sums[slot]


def second_kernel(
    boundary, rhs, v_ref, interior, partial, z_own, xa_own, xb_own, y_own,
    z_far, xa_far, xb_far, ya_far, yb_far, face_z, face_x, face_y,
    image, sums_out,
):
    odd_x, odd_y = odd_sides()
    edge = jnp.where(lax.axis_index("gz") == 0, NZ - 1, 0)
    sum_y = face_y[0] * y_own[...] + face_y[1] * pick_y(ya_far[...], yb_far[...])
    sum_xa = face_x[0, 0] * xa_own[...] + face_x[0, 1] * xa_far[...]
    sum_xb = face_x[1, 0] * xb_own[...] + face_x[1, 1] * xb_far[...]
    image[...] = interior[...]
    image[edge] = image[edge] + face_z[0] * z_own[...] + face_z[1] * z_far[...]

    sums = None
    for z in range(NZ):
        v = v_ref[z]
        total = image[z] + spread_sides(
            z, odd_x, odd_y, sum_xa[z : z + 1, :], sum_xb[z : z + 1, :], sum_y
        )
        plane = jnp.where(boundary[z] == 1, v, total)
        image[z] = plane
        products = [fold(p) for p in (plane * rhs[z], plane * v, plane * plane)]
        sums = products if z == 0 else [s + p for s, p in zip(sums, products, strict=True)]
    lane = lane_index((1, 8))
    row = jnp.zeros((1, 8), F32)
    for slot, part in enumerate([partial[0], partial[1], partial[2]] + sums):
        value = jnp.sum(jnp.sum(part, axis=0, keepdims=True), axis=1, keepdims=True)
        row = jnp.where(lane == slot, value, row)
    sums_out[...] = jnp.broadcast_to(row, sums_out.shape)


def combine_kernel(rhs, first, second, sums, update_out, residual_out, update, residual, left):
    total = jnp.sum(sums[...].reshape(-1, 8, 8), axis=0)
    total = jnp.sum(total, axis=0, keepdims=True)
    g00, g01, g11, g02, g12, g22 = (
        jnp.broadcast_to(total[:, i : i + 1], (8, 128)) for i in range(6)
    )
    over = 1.0 / (g00 + EPS)
    h00 = g01 * over
    rest = jnp.maximum((g11 - h00 * (2.0 * g01 - h00 * g00)) * over, 0.0)
    p = rest + EPS
    over_p = 1.0 / p
    over_n0 = 1.0 / (h00 * h00 + p)
    h01p = (g02 - h00 * g01) * over
    h11p = (g12 - h00 * (g02 + g11 - h00 * g01)) * over
    h11 = h11p * over_p
    h01_h01 = h01p * h01p * over_p
    norm_w = (g22 - h00 * (2.0 * g12 - h00 * g11)) * over * over_p
    v01p = (g01 - h00 * g00) * over
    last = norm_w + h01_h01 * (g00 * over - 2.0) + h11 * h11 * (rest * over_p - 2.0)
    last = last + 2.0 * (h01p * over_p) * h11 * v01p
    h21_h21 = jnp.maximum(last, 0.0) + EPS
    c = (h00 * h01p + h11p) * over_n0
    v0 = h01p - c * h00
    v1 = h11 - c
    n1 = v0 * v0 * over_p + v1 * v1 + h21_h21
    step = v0 * over_p / n1
    base = h00 * over_n0 - (c + h00) * step
    base, step = (
        jnp.concatenate([jnp.concatenate([x] * 2, axis=1)] * TILES, axis=0) for x in (base, step)
    )

    def plane_step(z, carry):
        a, b, c = rhs[z], first[z], second[z]
        update[z] = base * a + step * b
        residual[z] = a - (base * b + step * c)
        for slot, (source, target) in enumerate(pairs):
            pltpu.make_async_copy(source.at[z], target.at[z], left.at[slot, z]).start()
        return carry

    pairs = ((update, update_out), (residual, residual_out))
    lax.fori_loop(0, NZ, plane_step, 0)
    for z in range(NZ):
        for slot, (source, target) in enumerate(pairs):
            pltpu.make_async_copy(source.at[z], target.at[z], left.at[slot, z]).wait()


def cost(flops):
    return pl.CostEstimate(flops=flops, bytes_accessed=4 * 1024 * 1024, transcendentals=0)


def swap(x, axis, start, count):
    pairs = [(i, (i + 1) % count) for i in range(start, count, 2)]
    return lax.ppermute(x, axis, pairs + [(b, a) for a, b in pairs])


def exchange(z, xa, xb, y):
    count_x, count_y = lax.axis_size(GX), lax.axis_size(GY)
    return (
        swap(z, "gz", 0, 2),
        swap(xa, GX, 0, count_x),
        swap(xb, GX, 1, count_x),
        swap(y, GY, 0, count_y),
        swap(y, GY, 1, count_y),
    )


def call(kernel, ins, outs, flops, out_specs=None, scratch=()):
    return pl.pallas_call(
        kernel,
        out_shape=outs,
        in_specs=ins,
        out_specs=out_specs or tuple(VMEM for _ in outs),
        scratch_shapes=list(scratch),
        compiler_params=PARAMS,
        cost_estimate=cost(flops),
    )


def iterations(head, soil, boundary, rhs, soil_alpha, soil_n, soil_ks):
    whole = shape(*BLOCK)
    counts = jax.ShapeDtypeStruct(BLOCK, jnp.int32)
    sides = (shape(3, NX, NY), shape(3, 8, NY), shape(3, 8, NY), shape(3, 8, 128))
    sources = (head, soil, rhs, soil_alpha, soil_n, soil_ks, boundary)
    sources = [pltpu.with_memory_space_constraint(x, pltpu.HBM) for x in sources]
    head, soil, rhs, tables, z, xa, xb, y = call(
        pack_kernel,
        [HBM] * 6,
        (whole, counts, whole, shape(4, 8, 128)) + sides,
        1000000,
        scratch=[pltpu.SMEM((SOILS,), F32)] * 3 + [pltpu.SemaphoreType.DMA((6,))],
    )(*sources[:6])
    far = exchange(z, xa, xb, y)
    own = (shape(2, NX, NY), shape(2, 2, 8, NY), shape(2, 8, 128))
    coeffs, interior, own_z, own_x, own_y, boundary = call(
        terms_kernel,
        [VMEM] * 7 + [HBM],
        (shape(7, *BLOCK), whole) + own + (counts,),
        40000000,
        scratch=[pltpu.VMEM((NZ + 1, NX, NY), F32)] * 2 + [pltpu.SemaphoreType.DMA],
    )(head, soil, rhs, xa, xb, y, tables, sources[6])
    sides = (shape(NX, NY), shape(8, NY), shape(8, NY), shape(8, 128))
    first, z1, xa1, xb1, y1, face_z, face_x, face_y = call(
        first_kernel, [VMEM] * 17, (whole,) + sides + own, 8000000
    )(head, boundary, rhs, interior, z, xa, xb, y, own_z, own_x, own_y, *far, tables)
    far = exchange(z1, xa1, xb1, y1)
    interior, partial = call(inner_kernel, [VMEM] * 3, (whole, shape(3, 8, 128)), 8000000)(
        coeffs, first, rhs
    )
    second, sums = call(second_kernel, [VMEM] * 17, (whole, shape(256, 8)), 8000000)(
        boundary, rhs, first, interior, partial, z1, xa1, xb1, y1, *far, face_z, face_x, face_y
    )
    sums = lax.all_to_all(sums, AXES, 0, 0)
    return call(
        combine_kernel,
        [VMEM] * 4,
        (whole, whole),
        1000000,
        (HBM, HBM),
        [pltpu.VMEM(BLOCK, F32)] * 2 + [pltpu.SemaphoreType.DMA((2, NZ))],
    )(rhs, first, second, sums)


def solution(mesh):
    split = Mesh(mesh.devices.reshape(4, 4, 4, 2, mesh.shape["gz"]), AXES)
    in_specs = (P("gz", GX, GY),) * 4 + (P(), P(), P())
    out_specs = (P("gz", GX, GY), P("gz", GX, GY))
    return jax.shard_map(iterations, mesh=split, in_specs=in_specs, out_specs=out_specs, check_vma=False)
```

```python
import jax
import jax.numpy as jnp
from jax import lax
from jax.experimental import pallas as pl
from jax.experimental.pallas import tpu as pltpu
from jax.sharding import Mesh
from jax.sharding import PartitionSpec as P


AXES = ("gx_0", "gx_1", "gy_0", "gy_1", "gz")
GX = ("gx_0", "gx_1")
GY = ("gy_0", "gy_1")
SOILS = 8
EPS = 1e-06
SPEC = 0.0001
PORE = 0.4
STEP = 0.25
F32 = jnp.float32
LOG2E = 1.4426950408889634
NZ, NX, NY = 8, 64, 256
BLOCK = (NZ, NX, NY)
TILES = NX // 8
PARAMS = pltpu.CompilerParams(vmem_limit_bytes=24 * 1024 * 1024)
VMEM = pl.BlockSpec(memory_space=pltpu.VMEM)
HBM = pl.BlockSpec(memory_space=pltpu.HBM)


def shape(*dims):
    return jax.ShapeDtypeStruct(dims, F32)


def along(axes):
    index = lax.axis_index(axes[0])
    return index * lax.axis_size(axes[1]) + lax.axis_index(axes[1])


def pick(tables, soil):
    rows = []
    for row in range(0, soil.shape[0], 8):
        tiles = []
        for lane in range(0, soil.shape[1], 128):
            index = soil[row : row + 8, lane : lane + 128]
            tiles.append(
                [
                    jnp.take_along_axis(tables[t], index, axis=0, mode="promise_in_bounds")
                    for t in range(4)
                ]
            )
        rows.append([jnp.concatenate(x, axis=1) for x in zip(*tiles, strict=True)])
    return [jnp.concatenate(x, axis=0) for x in zip(*rows, strict=True)]


def cell_terms(head, soil, tables):
    minus_alpha, expo, ks, minus_power = pick(tables, soil)
    scaled = expo * jnp.log(minus_alpha * head)
    inverse = jnp.exp2(-LOG2E * scaled)
    total = 1.0 + inverse
    part = jnp.log(total)
    root = jnp.exp2(0.5 * (minus_power * (part + scaled)))
    bent = jnp.exp2(minus_power * part)
    rise = (1.0 - expo) / (head * total)
    gap = 1.0 - bent
    conduct = ks * root * gap
    cond = 2.0 * (conduct * gap)
    dcond = conduct * rise * (gap + 4.0 * (bent * inverse))
    capacity = root * root * (SPEC / STEP + (PORE / STEP) * rise)
    return cond, dcond, capacity


def couplings(k_own, dk_own, h_own, k_far, dk_far, h_far, tilt):
    part = 1.0 / (k_own + k_far)
    own, far = k_own * part, k_far * part
    slope = h_own - h_far
    if tilt is not None:
        slope = slope - tilt
    mean = far * k_own
    near = mean + far * far * (slope * dk_own)
    away = own * own * (slope * dk_far) - mean
    return near, away


def lane_index(dims):
    return lax.broadcasted_iota(jnp.int32, dims, len(dims) - 1)


def row_index(dims):
    return lax.broadcasted_iota(jnp.int32, dims, len(dims) - 2)


def gather_columns(plane, z):
    lane = lane_index((8, 128))
    packed = jnp.zeros((8, 128), F32)
    for tile in range(TILES):
        rows = slice(8 * tile, 8 * tile + 8)
        at = TILES * z + tile
        first = pltpu.roll(plane[rows, 0:128], at, axis=1) if at else plane[rows, 0:128]
        last = pltpu.roll(plane[rows, NY - 128 : NY], (at + 65) % 128, axis=1)
        packed = jnp.where(lane == at, first, packed)
        packed = jnp.where(lane == at + 64, last, packed)
    return packed


def column_lanes(odd_y):
    return jnp.where(odd_y, 0, 64), jnp.where(odd_y, 64, 0)


def add_columns(plane, z, first_at, last_at, packed):
    lane = lane_index((8, 128))
    for tile in range(TILES):
        rows = slice(8 * tile, 8 * tile + 8)
        first = jnp.broadcast_to(plane[rows, 0:1], (8, 128))
        last = jnp.broadcast_to(plane[rows, NY - 1 : NY], (8, 128))
        packed = jnp.where(lane == TILES * z + tile + first_at, first, packed)
        packed = jnp.where(lane == TILES * z + tile + last_at, last, packed)
    return packed


def tree(parts):
    while len(parts) > 1:
        parts = [a + b for a, b in zip(parts[::2], parts[1::2], strict=True)]
    return parts[0]


def by_phase(packed, odd_y):
    return jnp.where(odd_y, packed, pltpu.roll(packed, 64, axis=1))


def gather_rows(plane, odd_x):
    low, high = plane[0:1, :], plane[NX - 1 : NX, :]
    return jnp.where(odd_x, low, high), jnp.where(odd_x, high, low)


def spread_sides(z, odd_x, odd_y, row_a, row_b, packed):
    low, high = jnp.where(odd_x, row_a, row_b), jnp.where(odd_x, row_b, row_a)
    first = by_phase(packed, odd_y)
    lane, row = lane_index((8, 128)), row_index((8, NY))
    pieces = []
    for tile in range(TILES):
        at = TILES * z + tile
        left = pltpu.roll(first, (128 - at) % 128, axis=1)
        right = pltpu.roll(first, 63 - at, axis=1)
        left, right = jnp.where(lane == 0, left, 0.0), jnp.where(lane == 127, right, 0.0)
        piece = jnp.concatenate([left, right], axis=1)
        if tile == 0:
            piece = piece + jnp.where(row == 0, low, 0.0)
        if tile == TILES - 1:
            piece = piece + jnp.where(row == 7, high, 0.0)
        pieces.append(piece)
    return jnp.concatenate(pieces, axis=0)


def odd_sides():
    return (lax.axis_index("gx_1") % 2) == 1, lax.axis_index("gy_1") == 1


def pack_kernel(
    head, soil, rhs, alpha, expo, ks,
    head_out, soil_out, rhs_out, tables, z_out, xa_out, xb_out, y_out,
    alpha_in, expo_in, ks_in, arrived,
):
    pairs = (
        (alpha, alpha_in), (expo, expo_in), (ks, ks_in),
        (head, head_out), (soil, soil_out), (rhs, rhs_out),
    )
    copies = [
        pltpu.make_async_copy(source, target, arrived.at[i])
        for i, (source, target) in enumerate(pairs)
    ]
    for copy in copies:
        copy.start()
    odd_x, odd_y = odd_sides()
    edge = jnp.where(lax.axis_index("gz") == 0, NZ - 1, 0)
    first_at, last_at = column_lanes(odd_y)
    row = row_index((8, 128))
    lines = []
    for copy, source in zip(copies[:3], (alpha_in, expo_in, ks_in), strict=True):
        copy.wait()
        line = jnp.full((8, 128), source[0], F32)
        for entry in range(1, SOILS):
            line = jnp.where(row == entry, source[entry], line)
        lines.append(line)
    lines[0] = -lines[0]
    for slot, line in enumerate(lines + [LOG2E / lines[1] - LOG2E]):
        tables[slot] = line
    for slot, (copy, ref) in enumerate(
        zip(copies[3:6], (head_out, soil_out, rhs_out), strict=True)
    ):
        copy.wait()
        z_out[slot] = ref[edge].astype(F32)
        packed = jnp.zeros((8, 128), F32)
        for z in range(NZ):
            plane = ref[z].astype(F32)
            packed = add_columns(plane, z, first_at, last_at, packed)
            row_a, row_b = gather_rows(plane, odd_x)
            xa_out[slot, z : z + 1, :] = row_a
            xb_out[slot, z : z + 1, :] = row_b
        y_out[slot] = packed


def end_rows(x):
    tail = x[NX - 8 :, :]
    tail = jnp.where(row_index(tail.shape) < 7, tail, 0.0)
    return jnp.concatenate([x[: NX - 8, :], tail], axis=0)


def end_lanes(x):
    tail = x[:, NY - 128 :]
    tail = jnp.where(lane_index(tail.shape) < 127, tail, 0.0)
    return jnp.concatenate([x[:, : NY - 128], tail], axis=1)


def up(x, axis):
    return pltpu.roll(x, x.shape[axis] - 1, axis=axis)


def terms_kernel(
    head, soil, rhs, xa, xb, y, tables, boundary,
    coeffs, image, own_z, own_x, own_y, boundary_out, cond, dcond, arrived,
):
    copy = pltpu.make_async_copy(boundary, boundary_out, arrived)
    copy.start()
    edge = jnp.where(lax.axis_index("gz") == 0, NZ - 1, 0)

    def terms_step(z, carry):
        k, dk, capacity = cell_terms(head[z], soil[z], tables)
        cond[z], dcond[z], coeffs[0, z] = k, dk, capacity
        return carry

    lax.fori_loop(0, NZ, terms_step, 0)
    nothing = jnp.zeros((NX, NY), F32)
    cond[NZ], dcond[NZ] = nothing, nothing
    own_z[0], own_z[1] = cond[edge], dcond[edge]
    for slot, side in enumerate((xa, xb)):
        k, dk, _ = cell_terms(side[0], side[1].astype(jnp.int32), tables)
        own_x[slot, 0], own_x[slot, 1] = k, dk
    k, dk, _ = cell_terms(y[0], y[1].astype(jnp.int32), tables)
    own_y[0], own_y[1] = k, dk

    def faces_step(z, below):
        k, dk, h, v = cond[z], dcond[z], head[z], rhs[z]
        above = jnp.minimum(z + 1, NZ - 1)
        near, away = couplings(k, dk, h, cond[z + 1], dcond[z + 1], head[above], 1.0)
        coeffs[1, z], coeffs[2, z] = near, away
        flux = near * v + away * rhs[above]
        total = coeffs[0, z] * v + flux - below
        below = flux
        for slot, axis, end in ((3, 0, end_rows), (5, 1, end_lanes)):
            far = (end(up(k, axis)), end(up(dk, axis)), up(h, axis))
            near, away = couplings(k, dk, h, *far, None)
            coeffs[slot, z], coeffs[slot + 1, z] = near, away
            flux = near * v + away * up(v, axis)
            total = total + flux - pltpu.roll(flux, 1, axis=axis)
        image[z] = total
        return below

    lax.fori_loop(0, NZ, faces_step, nothing)
    copy.wait()


def pick_y(y_a, y_b):
    return jnp.where(lane_index(y_a.shape) < 64, y_a, y_b)


def first_kernel(
    head, boundary, rhs, interior, z_own, xa_own, xb_own, y_own, own_z, own_x, own_y,
    z_far, xa_far, xb_far, ya_far, yb_far, tables,
    image, z_out, xa_out, xb_out, y_out, face_z, face_x, face_y,
):
    odd_x, odd_y = odd_sides()
    gz = lax.axis_index("gz")
    edge = jnp.where(gz == 0, NZ - 1, 0)
    tilt = jnp.where(gz == 0, 1.0, -1.0)
    gx, gy = along(GX), along(GY)
    has_x = jnp.logical_and(gx > 0, gx < lax.axis_size(GX) - 1)
    has_y = jnp.logical_and(gy > 0, gy < lax.axis_size(GY) - 1)

    def face(own, own_terms, far, there, slant):
        far_head = far[0] if there is None else jnp.where(there, far[0], -1.0)
        k, dk, _ = cell_terms(far_head, far[1].astype(jnp.int32), tables)
        near, away = couplings(own_terms[0], own_terms[1], own[0], k, dk, far_head, slant)
        if there is not None:
            near, away = jnp.where(there, near, 0.0), jnp.where(there, away, 0.0)
        return near, away, near * own[2] + away * far[2]

    lane = lane_index((8, 128))
    far_y = tuple(pick_y(ya_far[slot], yb_far[slot]) for slot in range(3))
    there_y = jnp.logical_or(lane < 64, has_y)
    near, away, sum_y = face((y_own[0], None, y_own[2]), (own_y[0], own_y[1]), far_y, there_y, None)
    face_y[0], face_y[1] = near, away
    sums_x = []
    for slot, (own, far, there) in enumerate(((xa_own, xa_far, None), (xb_own, xb_far, has_x))):
        near, away, total = face(own, (own_x[slot, 0], own_x[slot, 1]), far, there, None)
        face_x[slot, 0], face_x[slot, 1] = near, away
        sums_x.append(total)
    near, away, sum_z = face(z_own, (own_z[0], own_z[1]), z_far, None, tilt)
    face_z[0], face_z[1] = near, away
    image[...] = interior[...]
    image[edge] = image[edge] + sum_z

    columns = []
    for z in range(NZ):
        total = image[z] + spread_sides(
            z, odd_x, odd_y, sums_x[0][z : z + 1, :], sums_x[1][z : z + 1, :], sum_y
        )
        plane = jnp.where(boundary[z] == 1, rhs[z], total)
        image[z] = plane
        row_a, row_b = gather_rows(plane, odd_x)
        xa_out[z : z + 1, :] = row_a
        xb_out[z : z + 1, :] = row_b
        columns.append(gather_columns(plane, z))
    y_out[...] = by_phase(tree(columns), odd_y)
    z_out[...] = image[edge]


def fold(x):
    total = x[0:8, 0:128] + x[0:8, 128:256]
    for tile in range(1, TILES):
        total = total + x[8 * tile : 8 * tile + 8, 0:128] + x[8 * tile : 8 * tile + 8, 128:256]
    return total


def inner_kernel(coeffs, v_ref, rhs, interior, partial):
    def plane_step(z, carry):
        below, sums = carry
        v, start = v_ref[z], rhs[z]
        above = jnp.minimum(z + 1, NZ - 1)
        flux = coeffs[1, z] * v + coeffs[2, z] * v_ref[above]
        total = coeffs[0, z] * v + flux - below
        below = flux
        for slot, axis in ((3, 0), (5, 1)):
            flux = coeffs[slot, z] * v + coeffs[slot + 1, z] * up(v, axis)
            total = total + flux - pltpu.roll(flux, 1, axis=axis)
        interior[z] = total
        products = (start * start, start * v, v * v)
        return below, tuple(s + fold(p) for s, p in zip(sums, products, strict=True))

    carry = jnp.zeros((NX, NY), F32), (jnp.zeros((8, 128), F32),) * 3
    _, sums = lax.fori_loop(0, NZ, plane_step, carry, unroll=True)
    for slot in range(3):
        partial[slot] = sums[slot]


def second_kernel(
    boundary, rhs, v_ref, interior, partial, z_own, xa_own, xb_own, y_own,
    z_far, xa_far, xb_far, ya_far, yb_far, face_z, face_x, face_y,
    image, sums_out,
):
    odd_x, odd_y = odd_sides()
    edge = jnp.where(lax.axis_index("gz") == 0, NZ - 1, 0)
    sum_y = face_y[0] * y_own[...] + face_y[1] * pick_y(ya_far[...], yb_far[...])
    sum_xa = face_x[0, 0] * xa_own[...] + face_x[0, 1] * xa_far[...]
    sum_xb = face_x[1, 0] * xb_own[...] + face_x[1, 1] * xb_far[...]
    image[...] = interior[...]
    image[edge] = image[edge] + face_z[0] * z_own[...] + face_z[1] * z_far[...]

    sums = None
    for z in range(NZ):
        v = v_ref[z]
        total = image[z] + spread_sides(
            z, odd_x, odd_y, sum_xa[z : z + 1, :], sum_xb[z : z + 1, :], sum_y
        )
        plane = jnp.where(boundary[z] == 1, v, total)
        image[z] = plane
        products = [fold(p) for p in (plane * rhs[z], plane * v, plane * plane)]
        sums = products if z == 0 else [s + p for s, p in zip(sums, products, strict=True)]
    lane = lane_index((1, 8))
    row = jnp.zeros((1, 8), F32)
    for slot, part in enumerate([partial[0], partial[1], partial[2]] + sums):
        value = jnp.sum(jnp.sum(part, axis=0, keepdims=True), axis=1, keepdims=True)
        row = jnp.where(lane == slot, value, row)
    sums_out[...] = jnp.broadcast_to(row, sums_out.shape)


def combine_kernel(rhs, first, second, sums, update_out, residual_out, update, residual, left):
    total = jnp.sum(sums[...].reshape(-1, 8, 8), axis=0)
    total = jnp.sum(total, axis=0, keepdims=True)
    g00, g01, g11, g02, g12, g22 = (
        jnp.broadcast_to(total[:, i : i + 1], (8, 128)) for i in range(6)
    )
    over = 1.0 / (g00 + EPS)
    h00 = g01 * over
    rest = jnp.maximum((g11 - h00 * (2.0 * g01 - h00 * g00)) * over, 0.0)
    p = rest + EPS
    over_p = 1.0 / p
    over_n0 = 1.0 / (h00 * h00 + p)
    h01p = (g02 - h00 * g01) * over
    h11p = (g12 - h00 * (g02 + g11 - h00 * g01)) * over
    h11 = h11p * over_p
    h01_h01 = h01p * h01p * over_p
    norm_w = (g22 - h00 * (2.0 * g12 - h00 * g11)) * over * over_p
    v01p = (g01 - h00 * g00) * over
    last = norm_w + h01_h01 * (g00 * over - 2.0) + h11 * h11 * (rest * over_p - 2.0)
    last = last + 2.0 * (h01p * over_p) * h11 * v01p
    h21_h21 = jnp.maximum(last, 0.0) + EPS
    c = (h00 * h01p + h11p) * over_n0
    v0 = h01p - c * h00
    v1 = h11 - c
    n1 = v0 * v0 * over_p + v1 * v1 + h21_h21
    step = v0 * over_p / n1
    base = h00 * over_n0 - (c + h00) * step
    base, step = (
        jnp.concatenate([jnp.concatenate([x] * 2, axis=1)] * TILES, axis=0) for x in (base, step)
    )

    def plane_step(z, carry):
        a, b, c = rhs[z], first[z], second[z]
        update[z] = base * a + step * b
        residual[z] = a - (base * b + step * c)
        for slot, (source, target) in enumerate(pairs):
            pltpu.make_async_copy(source.at[z], target.at[z], left.at[slot, z]).start()
        return carry

    pairs = ((update, update_out), (residual, residual_out))
    lax.fori_loop(0, NZ, plane_step, 0)
    for z in range(NZ):
        for slot, (source, target) in enumerate(pairs):
            pltpu.make_async_copy(source.at[z], target.at[z], left.at[slot, z]).wait()


def cost(flops):
    return pl.CostEstimate(flops=flops, bytes_accessed=4 * 1024 * 1024, transcendentals=0)


def swap(x, axis, start, count):
    pairs = [(i, (i + 1) % count) for i in range(start, count, 2)]
    return lax.ppermute(x, axis, pairs + [(b, a) for a, b in pairs])


def exchange(z, xa, xb, y):
    count_x, count_y = lax.axis_size(GX), lax.axis_size(GY)
    return (
        swap(z, "gz", 0, 2),
        swap(xa, GX, 0, count_x),
        swap(xb, GX, 1, count_x),
        swap(y, GY, 0, count_y),
        swap(y, GY, 1, count_y),
    )


def call(kernel, ins, outs, flops, out_specs=None, scratch=()):
    return pl.pallas_call(
        kernel,
        out_shape=outs,
        in_specs=ins,
        out_specs=out_specs or tuple(VMEM for _ in outs),
        scratch_shapes=list(scratch),
        compiler_params=PARAMS,
        cost_estimate=cost(flops),
    )


def iterations(head, soil, boundary, rhs, soil_alpha, soil_n, soil_ks):
    whole = shape(*BLOCK)
    counts = jax.ShapeDtypeStruct(BLOCK, jnp.int32)
    sides = (shape(3, NX, NY), shape(3, 8, NY), shape(3, 8, NY), shape(3, 8, 128))
    sources = (head, soil, rhs, soil_alpha, soil_n, soil_ks, boundary)
    sources = [pltpu.with_memory_space_constraint(x, pltpu.HBM) for x in sources]
    head, soil, rhs, tables, z, xa, xb, y = call(
        pack_kernel,
        [HBM] * 6,
        (whole, counts, whole, shape(4, 8, 128)) + sides,
        1000000,
        scratch=[pltpu.SMEM((SOILS,), F32)] * 3 + [pltpu.SemaphoreType.DMA((6,))],
    )(*sources[:6])
    far = exchange(z, xa, xb, y)
    own = (shape(2, NX, NY), shape(2, 2, 8, NY), shape(2, 8, 128))
    coeffs, interior, own_z, own_x, own_y, boundary = call(
        terms_kernel,
        [VMEM] * 7 + [HBM],
        (shape(7, *BLOCK), whole) + own + (counts,),
        40000000,
        scratch=[pltpu.VMEM((NZ + 1, NX, NY), F32)] * 2 + [pltpu.SemaphoreType.DMA],
    )(head, soil, rhs, xa, xb, y, tables, sources[6])
    sides = (shape(NX, NY), shape(8, NY), shape(8, NY), shape(8, 128))
    first, z1, xa1, xb1, y1, face_z, face_x, face_y = call(
        first_kernel, [VMEM] * 17, (whole,) + sides + own, 8000000
    )(head, boundary, rhs, interior, z, xa, xb, y, own_z, own_x, own_y, *far, tables)
    far = exchange(z1, xa1, xb1, y1)
    interior, partial = call(inner_kernel, [VMEM] * 3, (whole, shape(3, 8, 128)), 8000000)(
        coeffs, first, rhs
    )
    second, sums = call(second_kernel, [VMEM] * 17, (whole, shape(256, 8)), 8000000)(
        boundary, rhs, first, interior, partial, z1, xa1, xb1, y1, *far, face_z, face_x, face_y
    )
    sums = lax.all_to_all(sums, AXES, 0, 0)
    return call(
        combine_kernel,
        [VMEM] * 4,
        (whole, whole),
        1000000,
        (HBM, HBM),
        [pltpu.VMEM(BLOCK, F32)] * 2 + [pltpu.SemaphoreType.DMA((2, NZ))],
    )(rhs, first, second, sums)


def solution(mesh):
    split = Mesh(mesh.devices.reshape(4, 4, 4, 2, mesh.shape["gz"]), AXES)
    in_specs = (P("gz", GX, GY),) * 4 + (P(), P(), P())
    out_specs = (P("gz", GX, GY), P("gz", GX, GY))
    return jax.shard_map(iterations, mesh=split, in_specs=in_specs, out_specs=out_specs, check_vma=False)
```

```python
import jax
import jax.numpy as jnp
from jax import lax
from jax.experimental import pallas as pl
from jax.experimental.pallas import tpu as pltpu
from jax.sharding import Mesh
from jax.sharding import PartitionSpec as P


AXES = ("gx_0", "gx_1", "gy_0", "gy_1", "gz")
GX = ("gx_0", "gx_1")
GY = ("gy_0", "gy_1")
SOILS = 8
EPS = 1e-06
SPEC = 0.0001
PORE = 0.4
STEP = 0.25
F32 = jnp.float32
UNROLL = 8
LOG2E = 1.4426950408889634
NZ, NX, NY = 8, 64, 256
BLOCK = (NZ, NX, NY)
TILES = NX // 8
PARAMS = pltpu.CompilerParams(vmem_limit_bytes=24 * 1024 * 1024)
VMEM = pl.BlockSpec(memory_space=pltpu.VMEM)
HBM = pl.BlockSpec(memory_space=pltpu.HBM)


def shape(*dims):
    return jax.ShapeDtypeStruct(dims, F32)


def along(axes):
    index = lax.axis_index(axes[0])
    return index * lax.axis_size(axes[1]) + lax.axis_index(axes[1])


def pick(tables, soil):
    rows = []
    for row in range(0, soil.shape[0], 8):
        tiles = []
        for lane in range(0, soil.shape[1], 128):
            index = soil[row : row + 8, lane : lane + 128]
            tiles.append(
                [
                    jnp.take_along_axis(tables[t], index, axis=0, mode="promise_in_bounds")
                    for t in range(4)
                ]
            )
        rows.append([jnp.concatenate(x, axis=1) for x in zip(*tiles, strict=True)])
    return [jnp.concatenate(x, axis=0) for x in zip(*rows, strict=True)]


def cell_terms(head, soil, tables):
    minus_alpha, expo, ks, minus_power = pick(tables, soil)
    scaled = expo * jnp.log(minus_alpha * head)
    inverse = jnp.exp2(-LOG2E * scaled)
    total = 1.0 + inverse
    part = jnp.log(total)
    root = jnp.exp2(0.5 * (minus_power * (part + scaled)))
    bent = jnp.exp2(minus_power * part)
    rise = (1.0 - expo) / (head * total)
    gap = 1.0 - bent
    conduct = ks * root * gap
    cond = 2.0 * (conduct * gap)
    dcond = conduct * rise * (gap + 4.0 * (bent * inverse))
    capacity = root * root * (SPEC / STEP + (PORE / STEP) * rise)
    return cond, dcond, capacity


def couplings(k_own, dk_own, h_own, k_far, dk_far, h_far, tilt):
    part = 1.0 / (k_own + k_far)
    own, far = k_own * part, k_far * part
    slope = h_own - h_far
    if tilt is not None:
        slope = slope - tilt
    mean = far * k_own
    near = mean + far * far * (slope * dk_own)
    away = own * own * (slope * dk_far) - mean
    return near, away


def lane_index(dims):
    return lax.broadcasted_iota(jnp.int32, dims, len(dims) - 1)


def row_index(dims):
    return lax.broadcasted_iota(jnp.int32, dims, len(dims) - 2)


def gather_columns(plane, z):
    lane = lane_index((8, 128))
    packed = jnp.zeros((8, 128), F32)
    for tile in range(TILES):
        rows = slice(8 * tile, 8 * tile + 8)
        at = TILES * z + tile
        first = pltpu.roll(plane[rows, 0:128], at, axis=1) if at else plane[rows, 0:128]
        last = pltpu.roll(plane[rows, NY - 128 : NY], (at + 65) % 128, axis=1)
        packed = jnp.where(lane == at, first, packed)
        packed = jnp.where(lane == at + 64, last, packed)
    return packed


def column_lanes(odd_y):
    return jnp.where(odd_y, 0, 64), jnp.where(odd_y, 64, 0)


def add_columns(plane, z, first_at, last_at, packed):
    lane = lane_index((8, 128))
    for tile in range(TILES):
        rows = slice(8 * tile, 8 * tile + 8)
        first = jnp.broadcast_to(plane[rows, 0:1], (8, 128))
        last = jnp.broadcast_to(plane[rows, NY - 1 : NY], (8, 128))
        packed = jnp.where(lane == TILES * z + tile + first_at, first, packed)
        packed = jnp.where(lane == TILES * z + tile + last_at, last, packed)
    return packed


def tree(parts):
    while len(parts) > 1:
        parts = [a + b for a, b in zip(parts[::2], parts[1::2], strict=True)]
    return parts[0]


def by_phase(packed, odd_y):
    return jnp.where(odd_y, packed, pltpu.roll(packed, 64, axis=1))


def gather_rows(plane, odd_x):
    low, high = plane[0:1, :], plane[NX - 1 : NX, :]
    return jnp.where(odd_x, low, high), jnp.where(odd_x, high, low)


def spread_sides(z, odd_x, odd_y, row_a, row_b, packed):
    low, high = jnp.where(odd_x, row_a, row_b), jnp.where(odd_x, row_b, row_a)
    first = by_phase(packed, odd_y)
    lane, row = lane_index((8, 128)), row_index((8, NY))
    pieces = []
    for tile in range(TILES):
        at = TILES * z + tile
        left = pltpu.roll(first, (128 - at) % 128, axis=1)
        right = pltpu.roll(first, 63 - at, axis=1)
        left, right = jnp.where(lane == 0, left, 0.0), jnp.where(lane == 127, right, 0.0)
        piece = jnp.concatenate([left, right], axis=1)
        if tile == 0:
            piece = piece + jnp.where(row == 0, low, 0.0)
        if tile == TILES - 1:
            piece = piece + jnp.where(row == 7, high, 0.0)
        pieces.append(piece)
    return jnp.concatenate(pieces, axis=0)


def odd_sides():
    return (lax.axis_index("gx_1") % 2) == 1, lax.axis_index("gy_1") == 1


def pack_kernel(
    head, soil, rhs, alpha, expo, ks,
    head_out, soil_out, rhs_out, tables, z_out, xa_out, xb_out, y_out,
    alpha_in, expo_in, ks_in, arrived,
):
    pairs = (
        (alpha, alpha_in), (expo, expo_in), (ks, ks_in),
        (head, head_out), (soil, soil_out), (rhs, rhs_out),
    )
    copies = [
        pltpu.make_async_copy(source, target, arrived.at[i])
        for i, (source, target) in enumerate(pairs)
    ]
    for copy in copies:
        copy.start()
    odd_x, odd_y = odd_sides()
    edge = jnp.where(lax.axis_index("gz") == 0, NZ - 1, 0)
    first_at, last_at = column_lanes(odd_y)
    row = row_index((8, 128))
    lines = []
    for copy, source in zip(copies[:3], (alpha_in, expo_in, ks_in), strict=True):
        copy.wait()
        line = jnp.full((8, 128), source[0], F32)
        for entry in range(1, SOILS):
            line = jnp.where(row == entry, source[entry], line)
        lines.append(line)
    lines[0] = -lines[0]
    for slot, line in enumerate(lines + [LOG2E / lines[1] - LOG2E]):
        tables[slot] = line
    for slot, (copy, ref) in enumerate(
        zip(copies[3:6], (head_out, soil_out, rhs_out), strict=True)
    ):
        copy.wait()
        z_out[slot] = ref[edge].astype(F32)
        packed = jnp.zeros((8, 128), F32)
        for z in range(NZ):
            plane = ref[z].astype(F32)
            packed = add_columns(plane, z, first_at, last_at, packed)
            row_a, row_b = gather_rows(plane, odd_x)
            xa_out[slot, z : z + 1, :] = row_a
            xb_out[slot, z : z + 1, :] = row_b
        y_out[slot] = packed


def end_rows(x):
    tail = x[NX - 8 :, :]
    tail = jnp.where(row_index(tail.shape) < 7, tail, 0.0)
    return jnp.concatenate([x[: NX - 8, :], tail], axis=0)


def end_lanes(x):
    tail = x[:, NY - 128 :]
    tail = jnp.where(lane_index(tail.shape) < 127, tail, 0.0)
    return jnp.concatenate([x[:, : NY - 128], tail], axis=1)


def up(x, axis):
    return pltpu.roll(x, x.shape[axis] - 1, axis=axis)


def terms_kernel(
    head, soil, rhs, xa, xb, y, tables, boundary,
    coeffs, image, own_z, own_x, own_y, boundary_out, cond, dcond, arrived,
):
    copy = pltpu.make_async_copy(boundary, boundary_out, arrived)
    copy.start()
    edge = jnp.where(lax.axis_index("gz") == 0, NZ - 1, 0)

    def terms_step(z, carry):
        k, dk, capacity = cell_terms(head[z], soil[z], tables)
        cond[z], dcond[z], coeffs[0, z] = k, dk, capacity
        return carry

    lax.fori_loop(0, NZ, terms_step, 0)
    nothing = jnp.zeros((NX, NY), F32)
    cond[NZ], dcond[NZ] = nothing, nothing
    own_z[0], own_z[1] = cond[edge], dcond[edge]
    for slot, side in enumerate((xa, xb)):
        k, dk, _ = cell_terms(side[0], side[1].astype(jnp.int32), tables)
        own_x[slot, 0], own_x[slot, 1] = k, dk
    k, dk, _ = cell_terms(y[0], y[1].astype(jnp.int32), tables)
    own_y[0], own_y[1] = k, dk

    def faces_step(z, below):
        k, dk, h, v = cond[z], dcond[z], head[z], rhs[z]
        above = jnp.minimum(z + 1, NZ - 1)
        near, away = couplings(k, dk, h, cond[z + 1], dcond[z + 1], head[above], 1.0)
        coeffs[1, z], coeffs[2, z] = near, away
        flux = near * v + away * rhs[above]
        total = coeffs[0, z] * v + flux - below
        below = flux
        for slot, axis, end in ((3, 0, end_rows), (5, 1, end_lanes)):
            far = (end(up(k, axis)), end(up(dk, axis)), up(h, axis))
            near, away = couplings(k, dk, h, *far, None)
            coeffs[slot, z], coeffs[slot + 1, z] = near, away
            flux = near * v + away * up(v, axis)
            total = total + flux - pltpu.roll(flux, 1, axis=axis)
        image[z] = total
        return below

    lax.fori_loop(0, NZ, faces_step, nothing, unroll=UNROLL)
    copy.wait()


def pick_y(y_a, y_b):
    return jnp.where(lane_index(y_a.shape) < 64, y_a, y_b)


def first_kernel(
    head, boundary, rhs, interior, z_own, xa_own, xb_own, y_own, own_z, own_x, own_y,
    z_far, xa_far, xb_far, ya_far, yb_far, tables,
    image, z_out, xa_out, xb_out, y_out, face_z, face_x, face_y,
):
    odd_x, odd_y = odd_sides()
    gz = lax.axis_index("gz")
    edge = jnp.where(gz == 0, NZ - 1, 0)
    tilt = jnp.where(gz == 0, 1.0, -1.0)
    gx, gy = along(GX), along(GY)
    has_x = jnp.logical_and(gx > 0, gx < lax.axis_size(GX) - 1)
    has_y = jnp.logical_and(gy > 0, gy < lax.axis_size(GY) - 1)

    def face(own, own_terms, far, there, slant):
        far_head = far[0] if there is None else jnp.where(there, far[0], -1.0)
        k, dk, _ = cell_terms(far_head, far[1].astype(jnp.int32), tables)
        near, away = couplings(own_terms[0], own_terms[1], own[0], k, dk, far_head, slant)
        if there is not None:
            near, away = jnp.where(there, near, 0.0), jnp.where(there, away, 0.0)
        return near, away, near * own[2] + away * far[2]

    lane = lane_index((8, 128))
    far_y = tuple(pick_y(ya_far[slot], yb_far[slot]) for slot in range(3))
    there_y = jnp.logical_or(lane < 64, has_y)
    near, away, sum_y = face((y_own[0], None, y_own[2]), (own_y[0], own_y[1]), far_y, there_y, None)
    face_y[0], face_y[1] = near, away
    sums_x = []
    for slot, (own, far, there) in enumerate(((xa_own, xa_far, None), (xb_own, xb_far, has_x))):
        near, away, total = face(own, (own_x[slot, 0], own_x[slot, 1]), far, there, None)
        face_x[slot, 0], face_x[slot, 1] = near, away
        sums_x.append(total)
    near, away, sum_z = face(z_own, (own_z[0], own_z[1]), z_far, None, tilt)
    face_z[0], face_z[1] = near, away
    at_edge = {0: jnp.where(gz == 0, 0.0, sum_z), NZ - 1: jnp.where(gz == 0, sum_z, 0.0)}

    columns = []
    for z in range(NZ):
        total = interior[z] + at_edge[z] if z in at_edge else interior[z]
        total = total + spread_sides(
            z, odd_x, odd_y, sums_x[0][z : z + 1, :], sums_x[1][z : z + 1, :], sum_y
        )
        plane = jnp.where(boundary[z] == 1, rhs[z], total)
        image[z] = plane
        row_a, row_b = gather_rows(plane, odd_x)
        xa_out[z : z + 1, :] = row_a
        xb_out[z : z + 1, :] = row_b
        columns.append(gather_columns(plane, z))
    y_out[...] = by_phase(tree(columns), odd_y)
    z_out[...] = image[edge]


def fold(x):
    total = x[0:8, 0:128] + x[0:8, 128:256]
    for tile in range(1, TILES):
        total = total + x[8 * tile : 8 * tile + 8, 0:128] + x[8 * tile : 8 * tile + 8, 128:256]
    return total


def inner_kernel(coeffs, v_ref, rhs, interior, partial):
    def plane_step(z, carry):
        below, sums = carry
        v, start = v_ref[z], rhs[z]
        above = jnp.minimum(z + 1, NZ - 1)
        flux = coeffs[1, z] * v + coeffs[2, z] * v_ref[above]
        total = coeffs[0, z] * v + flux - below
        below = flux
        for slot, axis in ((3, 0), (5, 1)):
            flux = coeffs[slot, z] * v + coeffs[slot + 1, z] * up(v, axis)
            total = total + flux - pltpu.roll(flux, 1, axis=axis)
        interior[z] = total
        products = (start * start, start * v, v * v)
        return below, tuple(s + fold(p) for s, p in zip(sums, products, strict=True))

    carry = jnp.zeros((NX, NY), F32), (jnp.zeros((8, 128), F32),) * 3
    _, sums = lax.fori_loop(0, NZ, plane_step, carry, unroll=True)
    for slot in range(3):
        partial[slot] = sums[slot]


def second_kernel(
    boundary, rhs, v_ref, interior, partial, z_own, xa_own, xb_own, y_own,
    z_far, xa_far, xb_far, ya_far, yb_far, face_z, face_x, face_y,
    image, sums_out,
):
    odd_x, odd_y = odd_sides()
    gz = lax.axis_index("gz")
    sum_y = face_y[0] * y_own[...] + face_y[1] * pick_y(ya_far[...], yb_far[...])
    sum_xa = face_x[0, 0] * xa_own[...] + face_x[0, 1] * xa_far[...]
    sum_xb = face_x[1, 0] * xb_own[...] + face_x[1, 1] * xb_far[...]
    sum_z = face_z[0] * z_own[...] + face_z[1] * z_far[...]
    at_edge = {0: jnp.where(gz == 0, 0.0, sum_z), NZ - 1: jnp.where(gz == 0, sum_z, 0.0)}

    sums = None
    for z in range(NZ):
        v = v_ref[z]
        total = interior[z] + at_edge[z] if z in at_edge else interior[z]
        total = total + spread_sides(
            z, odd_x, odd_y, sum_xa[z : z + 1, :], sum_xb[z : z + 1, :], sum_y
        )
        plane = jnp.where(boundary[z] == 1, v, total)
        image[z] = plane
        products = [fold(p) for p in (plane * rhs[z], plane * v, plane * plane)]
        sums = products if z == 0 else [s + p for s, p in zip(sums, products, strict=True)]
    lane = lane_index((1, 8))
    row = jnp.zeros((1, 8), F32)
    for slot, part in enumerate([partial[0], partial[1], partial[2]] + sums):
        value = jnp.sum(jnp.sum(part, axis=0, keepdims=True), axis=1, keepdims=True)
        row = jnp.where(lane == slot, value, row)
    sums_out[...] = jnp.broadcast_to(row, sums_out.shape)


def combine_kernel(rhs, first, second, sums, update_out, residual_out, update, residual, left):
    total = jnp.sum(sums[...].reshape(-1, 8, 8), axis=0)
    total = jnp.sum(total, axis=0, keepdims=True)
    g00, g01, g11, g02, g12, g22 = (
        jnp.broadcast_to(total[:, i : i + 1], (8, 128)) for i in range(6)
    )
    over = 1.0 / (g00 + EPS)
    h00 = g01 * over
    rest = jnp.maximum((g11 - h00 * (2.0 * g01 - h00 * g00)) * over, 0.0)
    p = rest + EPS
    over_p = 1.0 / p
    over_n0 = 1.0 / (h00 * h00 + p)
    h01p = (g02 - h00 * g01) * over
    h11p = (g12 - h00 * (g02 + g11 - h00 * g01)) * over
    h11 = h11p * over_p
    h01_h01 = h01p * h01p * over_p
    norm_w = (g22 - h00 * (2.0 * g12 - h00 * g11)) * over * over_p
    v01p = (g01 - h00 * g00) * over
    last = norm_w + h01_h01 * (g00 * over - 2.0) + h11 * h11 * (rest * over_p - 2.0)
    last = last + 2.0 * (h01p * over_p) * h11 * v01p
    h21_h21 = jnp.maximum(last, 0.0) + EPS
    c = (h00 * h01p + h11p) * over_n0
    v0 = h01p - c * h00
    v1 = h11 - c
    n1 = v0 * v0 * over_p + v1 * v1 + h21_h21
    step = v0 * over_p / n1
    base = h00 * over_n0 - (c + h00) * step
    base, step = (
        jnp.concatenate([jnp.concatenate([x] * 2, axis=1)] * TILES, axis=0) for x in (base, step)
    )

    def plane_step(z, carry):
        a, b, c = rhs[z], first[z], second[z]
        update[z] = base * a + step * b
        residual[z] = a - (base * b + step * c)
        for slot, (source, target) in enumerate(pairs):
            pltpu.make_async_copy(source.at[z], target.at[z], left.at[slot, z]).start()
        return carry

    pairs = ((update, update_out), (residual, residual_out))
    lax.fori_loop(0, NZ, plane_step, 0)
    for z in range(NZ):
        for slot, (source, target) in enumerate(pairs):
            pltpu.make_async_copy(source.at[z], target.at[z], left.at[slot, z]).wait()


def cost(flops):
    return pl.CostEstimate(flops=flops, bytes_accessed=4 * 1024 * 1024, transcendentals=0)


def swap(x, axis, start, count):
    pairs = [(i, (i + 1) % count) for i in range(start, count, 2)]
    return lax.ppermute(x, axis, pairs + [(b, a) for a, b in pairs])


def exchange(z, xa, xb, y):
    count_x, count_y = lax.axis_size(GX), lax.axis_size(GY)
    return (
        swap(z, "gz", 0, 2),
        swap(xa, GX, 0, count_x),
        swap(xb, GX, 1, count_x),
        swap(y, GY, 0, count_y),
        swap(y, GY, 1, count_y),
    )


def call(kernel, ins, outs, flops, out_specs=None, scratch=()):
    return pl.pallas_call(
        kernel,
        out_shape=outs,
        in_specs=ins,
        out_specs=out_specs or tuple(VMEM for _ in outs),
        scratch_shapes=list(scratch),
        compiler_params=PARAMS,
        cost_estimate=cost(flops),
    )


def iterations(head, soil, boundary, rhs, soil_alpha, soil_n, soil_ks):
    whole = shape(*BLOCK)
    counts = jax.ShapeDtypeStruct(BLOCK, jnp.int32)
    sides = (shape(3, NX, NY), shape(3, 8, NY), shape(3, 8, NY), shape(3, 8, 128))
    sources = (head, soil, rhs, soil_alpha, soil_n, soil_ks, boundary)
    sources = [pltpu.with_memory_space_constraint(x, pltpu.HBM) for x in sources]
    head, soil, rhs, tables, z, xa, xb, y = call(
        pack_kernel,
        [HBM] * 6,
        (whole, counts, whole, shape(4, 8, 128)) + sides,
        1000000,
        scratch=[pltpu.SMEM((SOILS,), F32)] * 3 + [pltpu.SemaphoreType.DMA((6,))],
    )(*sources[:6])
    far = exchange(z, xa, xb, y)
    own = (shape(2, NX, NY), shape(2, 2, 8, NY), shape(2, 8, 128))
    coeffs, interior, own_z, own_x, own_y, boundary = call(
        terms_kernel,
        [VMEM] * 7 + [HBM],
        (shape(7, *BLOCK), whole) + own + (counts,),
        40000000,
        scratch=[pltpu.VMEM((NZ + 1, NX, NY), F32)] * 2 + [pltpu.SemaphoreType.DMA],
    )(head, soil, rhs, xa, xb, y, tables, sources[6])
    sides = (shape(NX, NY), shape(8, NY), shape(8, NY), shape(8, 128))
    first, z1, xa1, xb1, y1, face_z, face_x, face_y = call(
        first_kernel, [VMEM] * 17, (whole,) + sides + own, 8000000
    )(head, boundary, rhs, interior, z, xa, xb, y, own_z, own_x, own_y, *far, tables)
    far = exchange(z1, xa1, xb1, y1)
    interior, partial = call(inner_kernel, [VMEM] * 3, (whole, shape(3, 8, 128)), 8000000)(
        coeffs, first, rhs
    )
    second, sums = call(second_kernel, [VMEM] * 17, (whole, shape(256, 8)), 8000000)(
        boundary, rhs, first, interior, partial, z1, xa1, xb1, y1, *far, face_z, face_x, face_y
    )
    sums = lax.all_to_all(sums, AXES, 0, 0)
    return call(
        combine_kernel,
        [VMEM] * 4,
        (whole, whole),
        1000000,
        (HBM, HBM),
        [pltpu.VMEM(BLOCK, F32)] * 2 + [pltpu.SemaphoreType.DMA((2, NZ))],
    )(rhs, first, second, sums)


def solution(mesh):
    split = Mesh(mesh.devices.reshape(4, 4, 4, 2, mesh.shape["gz"]), AXES)
    in_specs = (P("gz", GX, GY),) * 4 + (P(), P(), P())
    out_specs = (P("gz", GX, GY), P("gz", GX, GY))
    return jax.shard_map(iterations, mesh=split, in_specs=in_specs, out_specs=out_specs, check_vma=False)
```
